32 devices in a mesh: row: 4 (over x, core), col: 8 (over z, y).
Axes of the slice: x: 2, y: 2, z: 4, core: 2. Of those that a mesh axis runs over, the one named last changes fastest.
Arguments:
- forcing: float32 [2, 1024, 2048], P(None, 'row', 'col'), may hold values from -6 to 6
- wave_index: int32 [1], replicated, may hold values from 12 to 27
- directions: int32 [32], replicated, may hold values from 0 to 63
- row_coupling: float32 [4, 4], replicated, may hold values from -1 to 2, as said below
- col_coupling: float32 [8, 8], replicated, may hold values from -1 to 2, as said below
- mode_coupling: float32 [256, 256], replicated, may hold values from -1 to 2, as said below
Outputs:
- field: float32 [2, 1024, 2048], P(None, 'row', 'col')
The draws below stay inside these ranges and needn't reach their ends.
Inputs may be any that keep to these rules, and one draw needn't show every extreme that they name: `row_coupling`: entries of a coarse correction factor. `col_coupling`: entries of a coarse correction factor. `mode_coupling`: entries of a coarse correction factor.
All inputs are finite; a program needn't handle non-finite values.
Results may differ from the reference program's by a relative error of at most 0.0003.
Values sent between devices are 32-bit elements; how exact they have to be, the bound alone decides.
No kernel may reach another device: no remote copies, remote signals or barrier semaphores. Data moves between devices by JAX's collectives and lax.ppermute only.
A program may use at most 64 MiB of HBM per device.

```python
import math
import jax
import jax.numpy as jnp
from jax import lax

S = 256
MODES = 32
ANGLES = 64
ITERS = 3
NA = 4
NB = 8
NX = 1024
NY = 2048
DOFS = 256


def coupling_draw(key, order):
    noise = jax.random.truncated_normal(key, -5.0, 5.0, (order, order), jnp.float32)
    return jnp.eye(order, dtype=jnp.float32) + 0.3 / math.sqrt(order) * noise


def draw_row_coupling(key, part):
    return coupling_draw(jax.random.fold_in(key, 11), NA)


def draw_col_coupling(key, part):
    return coupling_draw(jax.random.fold_in(key, 12), NB)


def draw_mode_coupling(key, part):
    return coupling_draw(jax.random.fold_in(key, 13), DOFS)


def with_ends(entries, key, least, top_value):
    spot = [jax.random.randint(jax.random.fold_in(key, axis), (), 0, length) for axis, length in enumerate(entries.shape)]
    widest = entries.shape.index(max(entries.shape))
    next_to = spot[:widest] + [(spot[widest] + 1) % entries.shape[widest]] + spot[widest + 1:]
    return entries.at[tuple(spot)].set(least).at[tuple(next_to)].set(top_value)


def steps_of(key, extent, pieces, low, high):
    def one(axis_at, shards_of):
        draws = jax.random.uniform(jax.random.fold_in(jax.random.fold_in(key, 6), axis_at), (shards_of,), jnp.float32, low / len(pieces), high / len(pieces))
        return jnp.repeat(jnp.exp(draws), extent[axis_at] // shards_of).reshape((-1,) + (1,) * (len(extent) - axis_at - 1))

    factor_of = one(*pieces[0])
    for cut in pieces[1:]:
        factor_of = factor_of * one(*cut)
    return factor_of


def centred(stream_key, dims, spread, limit, shards=(), held_as=jnp.bfloat16):
    entries = jax.random.normal(stream_key, dims, jnp.float32) * spread
    if len(shards) > 0:
        entries = steps_of(stream_key, dims, shards, -0.22, 0.18) * entries
    return jnp.clip(entries, min=-limit, max=limit).astype(held_as)


def setup_inputs(seed: int = 0) -> dict:
    arg_keys = jax.random.split(jax.random.key(seed), 7)
    forcing = centred(arg_keys[0], (2, NX, NY), 1.0, 6.0, ((1, 4), (2, 8)), jnp.float32)
    wave_index = jax.random.randint(arg_keys[1], (1,), 12, 28).astype(jnp.int32)
    directions = with_ends(jax.random.randint(arg_keys[2], (MODES,), 0, ANGLES), jax.random.fold_in(arg_keys[2], 1), 0, ANGLES - 1).astype(jnp.int32)
    row_coupling = draw_row_coupling(jax.random.fold_in(arg_keys[6], 71), 0)
    col_coupling = draw_col_coupling(jax.random.fold_in(arg_keys[6], 71), 0)
    mode_coupling = draw_mode_coupling(jax.random.fold_in(arg_keys[6], 71), 0)
    return {"forcing": forcing, "wave_index": wave_index, "directions": directions, "row_coupling": row_coupling, "col_coupling": col_coupling, "mode_coupling": mode_coupling}


HIGH = lax.Precision.HIGHEST
KAPPA_UNIT = 0.04
DAMPING = 0.5

def sine_table(width):
    index = jnp.arange(1, width + 1, dtype=jnp.int32)
    phase = index[:, None] * index[None, :] % (2 * width + 2)
    basis = math.sqrt(2.0 / (width + 1)) * jnp.sin(math.pi / (width + 1) * phase.astype(jnp.float32))
    values = 2.0 - 2.0 * jnp.cos(math.pi / (width + 1) * index.astype(jnp.float32))
    return (basis, values)

def inverse_symbol(values, kappa):
    shift = kappa * kappa
    real_part = values[:, None] + values[None, :] - shift
    imag_part = DAMPING * shift
    norm = real_part * real_part + imag_part * imag_part
    return (real_part / norm, imag_part / norm)

def solve_blocks(blocks, basis, inv_real, inv_imag):
    coeff = jnp.einsum('xp,caxby->capby', basis, blocks, precision=HIGH)
    coeff = jnp.einsum('capby,yq->capbq', coeff, basis, precision=HIGH)
    real_part = coeff[0] * inv_real[None, :, None, :] - coeff[1] * inv_imag[None, :, None, :]
    imag_part = coeff[0] * inv_imag[None, :, None, :] + coeff[1] * inv_real[None, :, None, :]
    coeff = jnp.stack([real_part, imag_part])
    coeff = jnp.einsum('px,capbq->caxbq', basis, coeff, precision=HIGH)
    return jnp.einsum('caxbq,qy->caxby', coeff, basis, precision=HIGH)

def robin(edge, inner, kappa):
    real_part = edge[0] - kappa * (edge[1] - inner[1])
    imag_part = edge[1] + kappa * (edge[0] - inner[0])
    return jnp.stack([real_part, imag_part])

def add_sides(forcing, top_g, bottom_g, left_g, right_g, width):
    source = forcing.at[:, 0::width, :].add(top_g)
    source = source.at[:, width - 1::width, :].add(bottom_g)
    source = source.at[:, :, 0::width].add(left_g)
    return source.at[:, :, width - 1::width].add(right_g)

def wave_tables(kappa, directions, width):
    position = jnp.arange(width, dtype=jnp.int32).astype(jnp.float32)
    ramp = (position + 0.5) / width
    windows = jnp.stack([1.0 - ramp, ramp])
    theta = 2.0 * math.pi / ANGLES * directions.astype(jnp.float32)
    phase_x = kappa * jnp.cos(theta)[:, None] * position[None, :]
    phase_y = kappa * jnp.sin(theta)[:, None] * position[None, :]
    across = jnp.stack([windows[:, None, :] * jnp.cos(phase_x)[None], -windows[:, None, :] * jnp.sin(phase_x)[None]])
    along = jnp.stack([windows[:, None, :] * jnp.cos(phase_y)[None], -windows[:, None, :] * jnp.sin(phase_y)[None]])
    return (across, along)

def contract(values, table):
    real_part = jnp.einsum('abs,kms->abkm', values[0], table[0], precision=HIGH) - jnp.einsum('abs,kms->abkm', values[1], table[1], precision=HIGH)
    imag_part = jnp.einsum('abs,kms->abkm', values[0], table[1], precision=HIGH) + jnp.einsum('abs,kms->abkm', values[1], table[0], precision=HIGH)
    return jnp.stack([real_part, imag_part])

def complex_product(first, second):
    return jnp.stack([first[0] * second[0] - first[1] * second[1], first[0] * second[1] + first[1] * second[0]])

def project(jump_top, jump_bottom, jump_left, jump_right, across, along):
    width = across.shape[-1]
    total = complex_product(across[:, :, :, 0][:, None, None, :, None, :], contract(jump_top, along)[:, :, :, None])
    total = total + complex_product(across[:, :, :, width - 1][:, None, None, :, None, :], contract(jump_bottom, along)[:, :, :, None])
    total = total + complex_product(along[:, :, :, 0][:, None, None, None, :, :], contract(jump_left, across)[:, :, :, :, None])
    total = total + complex_product(along[:, :, :, width - 1][:, None, None, None, :, :], contract(jump_right, across)[:, :, :, :, None])
    return total / math.sqrt(width)

def synthesize(coarse, across, along):
    count_a = coarse.shape[0]
    count_b = coarse.shape[1]
    modes = across.shape[2]
    parts = coarse.reshape(count_a, count_b, 2, 2, 2, modes)
    z_real = parts[:, :, 0]
    z_imag = parts[:, :, 1]
    x_real = across[0]
    x_imag = -across[1]
    v_real = jnp.einsum('kmx,abkjm->abxjm', x_real, z_real, precision=HIGH) - jnp.einsum('kmx,abkjm->abxjm', x_imag, z_imag, precision=HIGH)
    v_imag = jnp.einsum('kmx,abkjm->abxjm', x_real, z_imag, precision=HIGH) + jnp.einsum('kmx,abkjm->abxjm', x_imag, z_real, precision=HIGH)
    y_real = along[0]
    y_imag = -along[1]
    out_real = jnp.einsum('abxjm,jmy->axby', v_real, y_real, precision=HIGH) - jnp.einsum('abxjm,jmy->axby', v_imag, y_imag, precision=HIGH)
    out_imag = jnp.einsum('abxjm,jmy->axby', v_real, y_imag, precision=HIGH) + jnp.einsum('abxjm,jmy->axby', v_imag, y_real, precision=HIGH)
    return jnp.stack([out_real, out_imag]) / math.sqrt(modes)

def move(rows, axis, forward):
    length = rows.shape[axis]
    zero = jnp.zeros_like(lax.slice_in_dim(rows, 0, 1, axis=axis))
    if forward:
        return jnp.concatenate([zero, lax.slice_in_dim(rows, 0, length - 1, axis=axis)], axis=axis)
    return jnp.concatenate([lax.slice_in_dim(rows, 1, length, axis=axis), zero], axis=axis)

def reference(forcing, wave_index, directions, row_coupling, col_coupling, mode_coupling):
    kappa = KAPPA_UNIT * wave_index[0].astype(jnp.float32)
    basis, values = sine_table(S)
    inv_real, inv_imag = inverse_symbol(values, kappa)
    across, along = wave_tables(kappa, directions, S)
    field = jnp.zeros_like(forcing)
    top_g = jnp.zeros((2, NA, NY), jnp.float32)
    bottom_g = jnp.zeros((2, NA, NY), jnp.float32)
    left_g = jnp.zeros((2, NX, NB), jnp.float32)
    right_g = jnp.zeros((2, NX, NB), jnp.float32)

    def solve_one(block):
        return solve_blocks(block[:, None], basis, inv_real, inv_imag)[:, 0]
    for sweep in range(ITERS):
        source = forcing
        if sweep > 0:
            top_g = robin(move(field[:, S - 1::S, :], 1, True), move(field[:, S - 2::S, :], 1, True), kappa)
            bottom_g = robin(move(field[:, 0::S, :], 1, False), move(field[:, 1::S, :], 1, False), kappa)
            left_g = robin(move(field[:, :, S - 1::S], 2, True), move(field[:, :, S - 2::S], 2, True), kappa)
            right_g = robin(move(field[:, :, 0::S], 2, False), move(field[:, :, 1::S], 2, False), kappa)
            source = add_sides(forcing, top_g, bottom_g, left_g, right_g, S)
        blocks = source.reshape(2, NA, S, NB, S).transpose(1, 0, 2, 3, 4)
        half = lax.map(solve_one, blocks).transpose(1, 0, 2, 3, 4).reshape(2, NX, NY)
        jump_top = (move(half[:, S - 1::S, :], 1, True) - top_g).reshape(2, NA, NB, S)
        jump_bottom = (move(half[:, 0::S, :], 1, False) - bottom_g).reshape(2, NA, NB, S)
        jump_left = (move(half[:, :, S - 1::S], 2, True) - left_g).reshape(2, NA, S, NB).transpose(0, 1, 3, 2)
        jump_right = (move(half[:, :, 0::S], 2, False) - right_g).reshape(2, NA, S, NB).transpose(0, 1, 3, 2)
        proj = project(jump_top, jump_bottom, jump_left, jump_right, across, along)
        resid = proj.transpose(1, 2, 0, 3, 4, 5).reshape(NA, NB, DOFS)
        mixed = jnp.einsum('ij,jbl->ibl', row_coupling, resid, precision=HIGH)
        mixed = jnp.einsum('bc,icl->ibl', col_coupling, mixed, precision=HIGH)
        coarse = jnp.einsum('ibl,ml->ibm', mixed, mode_coupling, precision=HIGH)
        field = half + synthesize(coarse, across, along).reshape(2, NX, NY)
    return field
```

```python
import functools
import math

import jax
import jax.numpy as jnp
import numpy as np
from jax import lax
from jax.experimental import pallas as pl
from jax.experimental.pallas import tpu as pltpu
from jax.sharding import PartitionSpec as P

ANGLES = 64
KAPPA_UNIT = 0.04
DAMPING = 0.5
F32 = jnp.float32
BF16 = jnp.bfloat16
NN = (((1,), (0,)), ((), ()))
NT = (((1,), (1,)), ((), ()))
TN = (((0,), (0,)), ((), ()))
VMEM = pl.BlockSpec(memory_space=pltpu.VMEM)
SMEM = pl.BlockSpec(memory_space=pltpu.SMEM)


def split(a):
    if isinstance(a, tuple):
        return a
    high = a.astype(BF16)
    return high, (a - high.astype(F32)).astype(BF16)


def dot(a, b, dims=NN):
    ah, al = split(a)
    bh, bl = split(b)
    mul = functools.partial(lax.dot_general, dimension_numbers=dims, preferred_element_type=F32)
    return mul(ah, bh) + (mul(ah, bl) + mul(al, bh))


def cmul(a, b):
    return a[0] * b[0] - a[1] * b[1], a[0] * b[1] + a[1] * b[0]


def add(*terms):
    return sum(t[0] for t in terms[1:]) + terms[0][0], sum(t[1] for t in terms[1:]) + terms[0][1]


def sub(a, b):
    return a[0] - b[0], a[1] - b[1]


def sine_table(width):
    index = np.arange(1, width + 1)
    basis = np.sqrt(2.0 / (width + 1)) * np.sin(np.pi / (width + 1) * (np.outer(index, index) % (2 * width + 2)))
    values = 2.0 - 2.0 * np.cos(np.pi / (width + 1) * index)
    return basis.astype(np.float32), values.astype(np.float32)


def lanes(shape):
    return lax.broadcasted_iota(jnp.int32, shape, len(shape) - 1)


def parity(width):
    return (1 - 2 * (lanes((1, width)) & 1)).astype(F32)


def inverse_symbol(col_values, row_values, kappa):
    shift = kappa * kappa
    real = col_values + row_values - shift
    imag = DAMPING * shift
    norm = 1.0 / (real * real + imag * imag)
    return real * norm, imag * norm


def turn(z, half):
    sign = jnp.where(lanes((1, 2 * half)) < half, -1.0, 1.0)
    return sign * pltpu.roll(z, half, 1)


def contract(rows, table):
    count, half = rows[0].shape[0], table[0].shape[0] // 2
    out = dot(jnp.concatenate(rows, 0), table, NT)
    return out[:count] + turn(out[count:], half)


def first_kernel(wave, forcing, qh, ql, rows, lam_col, dirs, payload, spectrum, hat, along, *, width, modes, count):
    kappa = KAPPA_UNIT * wave[0].astype(F32)
    basis = (qh[...], ql[...])
    line = lanes((1, width)).astype(F32)
    ramp = (line + 0.5) / width
    windows = (1.0 - ramp, ramp)
    theta = 2.0 * math.pi / ANGLES * dirs[...]
    tables = []
    for speed in (jnp.cos(theta), jnp.sin(theta)):
        phase = kappa * speed[:, :1] * line
        cosine, sine = jnp.cos(phase), jnp.sin(phase)
        tables += [w * cosine for w in windows] + [-w * sine for w in windows]
    table = jnp.concatenate(tables, 0)
    along[...] = table[4 * modes :]
    hats = dot(table, basis)
    hat[...] = hats
    across_hat, along_hat = split(hats[: 4 * modes]), split(hats[4 * modes :])

    half_way = dot(forcing[...].reshape(2 * width, width), basis)
    coeff = [dot(basis, half_way[:width]), dot(basis, half_way[width:])]
    spectrum[0] = coeff[0]
    spectrum[1] = coeff[1]
    inv = inverse_symbol(lam_col[...], rows[4:5], kappa)
    coeff = [split(c) for c in cmul(coeff, inv)]
    weights = split(rows[...])
    out = []
    vectors = []
    for dims, table_hat in ((NN, along_hat), (NT, across_hat)):
        real, imag = dot(weights, coeff[0], dims), dot(weights, coeff[1], dims)
        edges = []
        for near, inner in ((0, 1), (2, 3)):
            e = real[near : near + 1], imag[near : near + 1]
            d = sub(e, (real[inner : inner + 1], imag[inner : inner + 1]))
            edges.append(e)
            vectors += [e[0] - kappa * d[1], e[1] + kappa * d[0]]
        rows_r = jnp.concatenate([edges[0][0], edges[1][0]] + [edges[0][0]] * 6, 0)
        rows_i = jnp.concatenate([edges[0][1], edges[1][1]] + [edges[0][1]] * 6, 0)
        proj = contract((rows_r, rows_i), table_hat)
        out += [proj[0:1], proj[1:2]]
    flat = jnp.concatenate(out + vectors, 1)
    payload[...] = jnp.broadcast_to(flat, payload.shape)


def second_kernel(
    wave, own, gathered, spectrum, hat, along, coupling, mode, qh, ql, rows, lam_col, dirs_row, field, *, width, modes, nb
):
    count = gathered.shape[0]
    kappa = KAPPA_UNIT * wave[0].astype(F32)
    unknowns = 8 * modes
    half = 2 * modes
    inv = inverse_symbol(lam_col[...], rows[4:5], kappa)
    inv_split = split(inv[0]), split(inv[1])
    sign = parity(width)
    q0, q1 = rows[0:1], rows[1:2]
    robin_weight = q0, kappa * (q0 - q1)
    diag_rows = split(jnp.concatenate([q0 * q0, sign * q0 * q0, q0 * (q0 - q1), sign * q0 * (q0 - q1)] * 2, 0))
    diag = dot(diag_rows, inv_split[0]), dot(diag_rows, inv_split[1])
    same = diag[0][0:1], diag[1][0:1]
    opposite = diag[0][1:2], diag[1][1:2]
    same_robin = diag[0][0:1] - kappa * diag[1][2:3], diag[1][0:1] + kappa * diag[0][2:3]
    opposite_robin = diag[0][1:2] - kappa * diag[1][3:4], diag[1][1:2] + kappa * diag[0][3:4]
    hats = hat[...]
    across_hat, along_hat = split(hats[: 2 * half]), split(hats[2 * half :])
    tables = {"t": along_hat, "b": along_hat, "l": across_hat, "r": across_hat}
    mode_split = split(mode[...])

    lane = lanes((1, 4 * modes))
    theta = 2.0 * math.pi / ANGLES * dirs_row[...]
    speeds = jnp.cos(theta), jnp.sin(theta)
    pick = lane // half, (lane // modes) % 2

    def wave_at(axis, x):
        ramp = (x + 0.5) / width
        window = jnp.where(pick[axis] == 0, 1.0 - ramp, ramp)
        phase = kappa * speeds[axis] * float(x)
        return window * jnp.cos(phase), -window * jnp.sin(phase)

    ends = {}
    for side, axis, near, inner in (("t", 0, 0, 1), ("b", 0, width - 1, width - 2), ("l", 1, 0, 1), ("r", 1, width - 1, width - 2)):
        e, n = wave_at(axis, near), wave_at(axis, inner)
        er, ei, nr, ni = e[0], -e[1], n[0], -n[1]
        ends[side] = e, (er - kappa * (ei - ni), ei + kappa * (er - nr))
    facing = {"t": "b", "b": "t", "l": "r", "r": "l"}

    def spread(proj, side):
        low = lane < half
        if side in "tb":
            real = jnp.where(low, proj, pltpu.roll(proj, half, 1))
            imag = jnp.where(low, pltpu.roll(proj, half, 1), proj)
        else:
            by1, by2, by3 = (pltpu.roll(proj, k * modes, 1) for k in (1, 2, 3))
            block = lane // modes
            real = jnp.where(block == 0, proj, jnp.where(block == 3, by2, by1))
            imag = jnp.where(block == 0, by2, jnp.where(block == 3, proj, by3))
        parts = cmul((real, imag), ends[facing[side]][0])
        return jnp.concatenate(parts, 1)

    def outgoing(c, side):
        z = cmul((c[:, : unknowns // 2], c[:, unknowns // 2 :]), ends[side][1])
        low = lane < half
        if side in "tb":
            z = [a + pltpu.roll(a, half, 1) for a in z]
            z = jnp.where(low, z[0], z[1])
        else:
            z = [a + pltpu.roll(a, 3 * modes, 1) for a in z]
            block = lane // modes
            back = pltpu.roll(z[0], 3 * modes, 1)
            ahead = pltpu.roll(z[1], modes, 1)
            z = jnp.where(
                block == 0, z[0], jnp.where(block == 1, back, jnp.where(block == 2, pltpu.roll(z[1], 2 * modes, 1), ahead))
            )
        return z

    def synth(zs, table):
        size = zs[0].shape[0]
        stacked = jnp.concatenate([a for z in zs for a in (z, -turn(z, half))], 0)
        out = dot(stacked, table)
        return [(out[2 * k * size : (2 * k + 1) * size], out[(2 * k + 1) * size : (2 * k + 2) * size]) for k in range(len(zs))]

    def coarse_of(projs):
        total = 0.0
        for k, side in enumerate("tblr"):
            total = total + dot(coupling[k], spread(projs[side], side))
        return dot(total, mode_split, NT)

    def robin_of(c, base):
        tb = synth([outgoing(c, "t"), outgoing(c, "b")], along_hat)
        lr = synth([outgoing(c, "l"), outgoing(c, "r")], across_hat)
        return {side: add(base[side], s) for side, s in zip("tblr", tb + lr)}

    row = lax.broadcasted_iota(jnp.int32, (count, 1), 0)
    first, last = row % nb == 0, row % nb == nb - 1

    def incoming(out):
        zero = jnp.zeros((nb, width), F32)
        down = lambda a: jnp.concatenate([zero, a[:-nb]], 0)
        up = lambda a: jnp.concatenate([a[nb:], zero], 0)
        right = lambda a: jnp.where(first, 0.0, pltpu.roll(a, 1, 0))
        left = lambda a: jnp.where(last, 0.0, pltpu.roll(a, count - 1, 0))
        move = lambda f, z: (f(z[0]), f(z[1]))
        return {"t": move(down, out["b"]), "b": move(up, out["t"]), "l": move(right, out["r"]), "r": move(left, out["l"])}

    def apply_inverse(vectors):
        size = vectors[0][0].shape[0]
        k = len(vectors)
        stacked = split(jnp.concatenate([v[0] for v in vectors] + [v[1] for v in vectors], 0))
        a, b = dot(stacked, inv_split[0]), dot(stacked, inv_split[1])
        real, imag = a[: k * size] - b[k * size :], a[k * size :] + b[: k * size]
        return [(real[j * size : (j + 1) * size], imag[j * size : (j + 1) * size]) for j in range(k)]

    def scale(r, z):
        return r * z[0], r * z[1]

    def responses(g):
        edge, rob = {}, {}
        for (a, b), (c, d) in ((("t", "b"), ("l", "r")), (("l", "r"), ("t", "b"))):
            vectors = []
            for src in (a, b):
                plain, heavy = scale(q0, g[src]), cmul(g[src], robin_weight)
                vectors += [plain, scale(sign, plain), heavy, scale(sign, heavy)]
            x = apply_inverse(vectors)
            cross = [scale(q0, add(x[k], scale(sign, x[k + 4]))) for k in range(4)]
            edge[c], edge[d], rob[c], rob[d] = cross
        for a, b in (("t", "b"), ("l", "r")):
            edge[a] = add(edge[a], cmul(g[a], same), cmul(g[b], opposite))
            edge[b] = add(edge[b], cmul(g[b], same), cmul(g[a], opposite))
            rob[a] = add(rob[a], cmul(g[a], same_robin), cmul(g[b], opposite_robin))
            rob[b] = add(rob[b], cmul(g[b], same_robin), cmul(g[a], opposite_robin))
        return edge, rob

    values = gathered[...]
    lanes_of = 4 * modes
    proj0 = {s: values[:, k * lanes_of : (k + 1) * lanes_of] for k, s in enumerate("tblr")}
    at = 4 * lanes_of
    robin0 = {}
    for s in "tblr":
        robin0[s] = values[:, at : at + width], values[:, at + width : at + 2 * width]
        at += 2 * width

    out1 = robin_of(coarse_of(proj0), robin0)
    edge, rob = responses(incoming(out1))
    proj1 = {}
    for a, b in (("t", "b"), ("l", "r")):
        ja, jb = sub(edge[a], out1[a]), sub(edge[b], out1[b])
        both = contract((jnp.concatenate([ja[0], jb[0]], 0), jnp.concatenate([ja[1], jb[1]], 0)), tables[a])
        proj1[a], proj1[b] = proj0[a] + both[:count], proj0[b] + both[count:]
    base = {s: add(robin0[s], rob[s]) for s in "tblr"}
    out2 = robin_of(coarse_of(proj1), base)
    g2 = incoming(out2)

    mine = own[0]
    picks = [coupling[k, pl.ds(mine, 1), :] for k in range(4)]
    one = (lanes((1, count)) == mine).astype(F32)
    weights = split(jnp.concatenate(picks + [one] * 4, 0))
    mixed = {s: (dot(weights, g2[s][0]), dot(weights, g2[s][1])) for s in "tblr"}
    sent = {s: (dot(weights, out2[s][0]), dot(weights, out2[s][1])) for s in "tblr"}
    base0 = {s: dot(weights, proj0[s]) for s in "tblr"}
    index = {"t": 0, "b": 1, "l": 2, "r": 3}
    rowof = lambda z, k: (z[0][k : k + 1], z[1][k : k + 1])
    vectors = []
    order = []
    for o in "tblr":
        weight = scale(sign, (q0, q0)) if o in "br" else (q0, q0)
        for src in ("lr" if o in "tb" else "tb"):
            z = rowof(mixed[src], index[o])
            vectors.append((weight[0] * z[0], weight[0] * z[1]))
            order.append((o, src))
    x = apply_inverse(vectors)
    total = jnp.zeros((1, unknowns), F32)
    jumps = {}
    for o in "tblr":
        k = 2 * index[o]
        e = scale(q0, add(x[k], scale(sign, x[k + 1])))
        e = add(e, cmul(rowof(mixed[o], index[o]), same), cmul(rowof(mixed[facing[o]], index[o]), opposite))
        jumps[o] = sub(e, rowof(sent[o], index[o]))
    for a, b in (("t", "b"), ("l", "r")):
        rr = jnp.concatenate([jumps[a][0], jumps[b][0]] + [jumps[a][0]] * 6, 0)
        ri = jnp.concatenate([jumps[a][1], jumps[b][1]] + [jumps[a][1]] * 6, 0)
        both = contract((rr, ri), tables[a])
        for j, o in enumerate((a, b)):
            k = index[o]
            total = total + spread(base0[o][k : k + 1] + both[j : j + 1], o)
    c2 = dot(jnp.broadcast_to(total, (8, unknowns)), mode_split, NT)[0:1]

    mine_g = {s: rowof(mixed[s], 4) for s in "tblr"}
    basis = (qh[...], ql[...])
    coeff = []
    zero = jnp.zeros((4, width), F32)
    sq0 = sign * q0
    for part in range(2):
        left_rows = jnp.concatenate([q0, sq0, mine_g["l"][part], mine_g["r"][part], zero], 0)
        right_rows = jnp.concatenate([mine_g["t"][part], mine_g["b"][part], q0, sq0, zero], 0)
        coeff.append(spectrum[part] + dot(left_rows, right_rows, TN))
    coeff = cmul(coeff, inv)
    half_way = [dot(basis, coeff[0]), dot(basis, coeff[1])]

    cr, ci = c2[:, : 4 * modes], c2[:, 4 * modes :]
    low = lane < half
    flip = lambda a: pltpu.roll(a, half, 1)
    a0, a1 = jnp.where(low, cr, flip(ci)), jnp.where(low, flip(cr), ci)
    line = lax.broadcasted_iota(jnp.int32, (width, 1), 0).astype(F32)
    ramp = (line + 0.5) / width
    phase = kappa * speeds[0] * line
    plain = (1.0 - ramp) * a0 + ramp * a1
    turned = (1.0 - ramp) * turn(a0, half) + ramp * turn(a1, half)
    v = jnp.cos(phase) * plain + jnp.sin(phase) * turned
    along_split = split(along[...])
    field[0] = dot(half_way[0], basis) + dot(v, along_split)
    field[1] = dot(half_way[1], basis) + dot(-turn(v, half), along_split)


def local(forcing, wave_index, directions, row_coupling, col_coupling, mode_coupling):
    width = forcing.shape[1]
    modes = directions.shape[0]
    na, nb = row_coupling.shape[0], col_coupling.shape[0]
    count = na * nb
    size = 4 * 4 * modes + 4 * 2 * width
    basis, values = sine_table(width)
    qh = basis.astype(jnp.bfloat16)
    ql = (basis - qh.astype(np.float32)).astype(jnp.bfloat16)
    sign = 1.0 - 2.0 * (np.arange(width) % 2)
    rows = np.zeros((8, width), np.float32)
    rows[0], rows[1], rows[2], rows[3], rows[4] = basis[0], basis[1], sign * basis[0], sign * basis[1], values
    lam_col = np.ascontiguousarray(values[:, None])
    turns = directions.astype(F32)
    dirs = jnp.broadcast_to(turns[:, None], (modes, 128))
    dirs_row = jnp.tile(turns, 4)[None, :]

    scale = 1.0 / math.sqrt(width) / math.sqrt(modes)
    rc, cc = row_coupling * scale, col_coupling
    pad = lambda m, lo: jnp.pad(m[:, :-1] if lo else m[:, 1:], ((0, 0), (1, 0) if lo else (0, 1)))
    kron = lambda a, b: (a[:, None, :, None] * b[None, :, None, :]).reshape(count, count)
    coupling = jnp.stack([kron(pad(rc, True), cc), kron(pad(rc, False), cc), kron(rc, pad(cc, True)), kron(rc, pad(cc, False))])
    own = (lax.axis_index("row") * nb + lax.axis_index("col")).reshape(1)

    payload, spectrum, hat, along = pl.pallas_call(
        functools.partial(first_kernel, width=width, modes=modes, count=count),
        out_shape=[
            jax.ShapeDtypeStruct((count, size), F32),
            jax.ShapeDtypeStruct((2, width, width), F32),
            jax.ShapeDtypeStruct((8 * modes, width), F32),
            jax.ShapeDtypeStruct((4 * modes, width), F32),
        ],
        in_specs=[SMEM] + [VMEM] * 6,
        out_specs=[VMEM] * 4,
        name="spectrum",
    )(wave_index, forcing, qh, ql, rows, lam_col, dirs)
    gathered = lax.all_to_all(payload, ("row", "col"), 0, 0, tiled=True)
    return pl.pallas_call(
        functools.partial(second_kernel, width=width, modes=modes, nb=nb),
        out_shape=jax.ShapeDtypeStruct((2, width, width), F32),
        in_specs=[SMEM, SMEM] + [VMEM] * 10 + [VMEM],
        out_specs=VMEM,
        name="sweeps",
    )(wave_index, own, gathered, spectrum, hat, along, coupling, mode_coupling, qh, ql, rows, lam_col, dirs_row)


def solution(mesh):
    return jax.shard_map(
        local,
        mesh=mesh,
        in_specs=(P(None, "row", "col"), P(), P(), P(), P(), P()),
        out_specs=P(None, "row", "col"),
        check_vma=False,
    )
```

```python
import functools
import math

import jax
import jax.numpy as jnp
import numpy as np
from jax import lax
from jax.experimental import pallas as pl
from jax.experimental.pallas import tpu as pltpu
from jax.sharding import PartitionSpec as P

ANGLES = 64
KAPPA_UNIT = 0.04
DAMPING = 0.5
F32 = jnp.float32
BF16 = jnp.bfloat16
NN = (((1,), (0,)), ((), ()))
NT = (((1,), (1,)), ((), ()))
TN = (((0,), (0,)), ((), ()))
VMEM = pl.BlockSpec(memory_space=pltpu.VMEM)
HBM = pl.BlockSpec(memory_space=pltpu.HBM)
SMEM = pl.BlockSpec(memory_space=pltpu.SMEM)


def split(a):
    if isinstance(a, tuple):
        return a
    high = a.astype(BF16)
    return high, (a - high.astype(F32)).astype(BF16)


def dot(a, b, dims=NN):
    ah, al = split(a)
    bh, bl = split(b)
    mul = functools.partial(lax.dot_general, dimension_numbers=dims, preferred_element_type=F32)
    return mul(ah, bh) + (mul(ah, bl) + mul(al, bh))


def cmul(a, b):
    return a[0] * b[0] - a[1] * b[1], a[0] * b[1] + a[1] * b[0]


def add(*terms):
    return sum(t[0] for t in terms[1:]) + terms[0][0], sum(t[1] for t in terms[1:]) + terms[0][1]


def sub(a, b):
    return a[0] - b[0], a[1] - b[1]


def sine_table(width):
    index = np.arange(1, width + 1)
    basis = np.sqrt(2.0 / (width + 1)) * np.sin(np.pi / (width + 1) * (np.outer(index, index) % (2 * width + 2)))
    values = 2.0 - 2.0 * np.cos(np.pi / (width + 1) * index)
    return basis.astype(np.float32), values.astype(np.float32)


def lanes(shape):
    return lax.broadcasted_iota(jnp.int32, shape, len(shape) - 1)


def parity(width):
    return (1 - 2 * (lanes((1, width)) & 1)).astype(F32)


def inverse_symbol(col_values, row_values, kappa):
    shift = kappa * kappa
    real = col_values + row_values - shift
    imag = DAMPING * shift
    norm = 1.0 / (real * real + imag * imag)
    return real * norm, imag * norm


def turn(z, half):
    sign = jnp.where(lanes((1, 2 * half)) < half, -1.0, 1.0)
    return sign * pltpu.roll(z, half, 1)


def contract(rows, table):
    count, half = rows[0].shape[0], table[0].shape[0] // 2
    out = dot(jnp.concatenate(rows, 0), table, NT)
    return out[:count] + turn(out[count:], half)


def turn_column(dirs, modes):
    shape = (modes, modes)
    spot = lax.broadcasted_iota(jnp.int32, shape, 0) == lanes(shape)
    column = jnp.sum(jnp.where(spot, jnp.broadcast_to(dirs[...].astype(F32), shape), 0.0), 1, keepdims=True)
    return 2.0 * math.pi / ANGLES * column


def turn_row(dirs, modes):
    shape = (modes, 4 * modes)
    spot = (lax.broadcasted_iota(jnp.int32, shape, 0) == lanes(shape) % modes).astype(F32)
    row = lax.dot_general(
        jnp.broadcast_to(dirs[...].astype(F32), (8, modes)).astype(BF16), spot.astype(BF16), NN, preferred_element_type=F32
    )
    return 2.0 * math.pi / ANGLES * row[0:1]


def first_kernel(
    wave_in, dirs_in, forcing_in, qh_in, ql_in, rows_in, lam_in, payload_out, spectrum_out, hat_out, along_out,
    wave, dirs, forcing, qh, ql, rows, lam_col, payload, spectrum, hat, along, arrived, left, *, width, modes, count
):
    sources = wave_in, dirs_in, qh_in, ql_in, forcing_in, rows_in, lam_in
    targets = wave, dirs, qh, ql, forcing, rows, lam_col
    copies = [pltpu.make_async_copy(a, b, arrived.at[k]) for k, (a, b) in enumerate(zip(sources, targets))]
    for copy in copies:
        copy.start()
    for copy in copies[:2]:
        copy.wait()
    kappa = KAPPA_UNIT * wave[...].astype(F32)
    line = lanes((1, width)).astype(F32)
    ramp = (line + 0.5) / width
    windows = (1.0 - ramp, ramp)
    theta = turn_column(dirs, modes)
    tables = []
    for speed in (jnp.cos(theta), jnp.sin(theta)):
        phase = kappa * speed * line
        cosine, sine = jnp.cos(phase), jnp.sin(phase)
        tables += [w * cosine for w in windows] + [-w * sine for w in windows]
    table = jnp.concatenate(tables, 0)
    along[...] = table[4 * modes :]
    sends = [
        pltpu.make_async_copy(a, b, left.at[k])
        for k, (a, b) in enumerate(((along, along_out), (hat, hat_out), (spectrum, spectrum_out), (payload, payload_out)))
    ]
    sends[0].start()
    for copy in copies[2:]:
        copy.wait()
    basis = (qh[...], ql[...])
    hats = split(dot(table, basis))
    hat[0], hat[1] = hats
    sends[1].start()
    across_hat = hats[0][: 4 * modes], hats[1][: 4 * modes]
    along_hat = hats[0][4 * modes :], hats[1][4 * modes :]

    half_way = dot(forcing[...].reshape(2 * width, width), basis)
    coeff = [dot(basis, half_way[:width]), dot(basis, half_way[width:])]
    spectrum[0] = coeff[0]
    spectrum[1] = coeff[1]
    sends[2].start()
    inv = inverse_symbol(lam_col[...], rows[4:5], kappa)
    coeff = [split(c) for c in cmul(coeff, inv)]
    weights = split(rows[...])
    out = []
    vectors = []
    for dims, table_hat in ((NN, along_hat), (NT, across_hat)):
        real, imag = dot(weights, coeff[0], dims), dot(weights, coeff[1], dims)
        edges = []
        for near, inner in ((0, 1), (2, 3)):
            e = real[near : near + 1], imag[near : near + 1]
            d = sub(e, (real[inner : inner + 1], imag[inner : inner + 1]))
            edges.append(e)
            vectors += [e[0] - kappa * d[1], e[1] + kappa * d[0]]
        rows_r = jnp.concatenate([edges[0][0], edges[1][0]] + [edges[0][0]] * 6, 0)
        rows_i = jnp.concatenate([edges[0][1], edges[1][1]] + [edges[0][1]] * 6, 0)
        proj = contract((rows_r, rows_i), table_hat)
        out += [proj[0:1], proj[1:2]]
    flat = jnp.concatenate(out + vectors, 1)
    payload[...] = jnp.broadcast_to(flat[None], payload.shape)
    sends[3].start()
    for copy in sends:
        copy.wait()


def table_kernel(wave, mode, rows, lam_col, dirs, inv_out, diag_out, ends_out, mode_out, wave_out, *, width, modes):
    kappa = KAPPA_UNIT * wave[...].astype(F32)
    half = 2 * modes
    inv = inverse_symbol(lam_col[...], rows[4:5], kappa)
    inv_split = split(inv[0]), split(inv[1])
    for part in range(2):
        for k in range(2):
            inv_out[2 * part + k] = inv_split[part][k]
    sign = parity(width)
    q0, q1 = rows[0:1], rows[1:2]
    diag_rows = split(jnp.concatenate([q0 * q0, sign * q0 * q0, q0 * (q0 - q1), sign * q0 * (q0 - q1)] * 2, 0))
    real, imag = dot(diag_rows, inv_split[0]), dot(diag_rows, inv_split[1])
    diag_out[...] = jnp.concatenate(
        [
            real[0:1], imag[0:1], real[1:2], imag[1:2],
            real[0:1] - kappa * imag[2:3], imag[0:1] + kappa * real[2:3],
            real[1:2] - kappa * imag[3:4], imag[1:2] + kappa * real[3:4],
        ],
        0,
    )
    mode_out[0], mode_out[1] = split(mode[...])

    lane = lanes((1, 4 * modes))
    theta = turn_row(dirs, modes)
    speeds = jnp.cos(theta), jnp.sin(theta)
    pick = lane // half, (lane // modes) % 2

    def wave_at(axis, x):
        ramp = (x + 0.5) / width
        window = jnp.where(pick[axis] == 0, 1.0 - ramp, ramp)
        phase = kappa * speeds[axis] * float(x)
        return window * jnp.cos(phase), -window * jnp.sin(phase)

    ends = []
    for axis, near, inner in ((0, 0, 1), (0, width - 1, width - 2), (1, 0, 1), (1, width - 1, width - 2)):
        e, n = wave_at(axis, near), wave_at(axis, inner)
        er, ei, nr, ni = e[0], -e[1], n[0], -n[1]
        ends += [e[0], e[1], er - kappa * (ei - ni), ei + kappa * (er - nr)]
    ends_out[...] = jnp.concatenate(ends, 0)
    line = lax.broadcasted_iota(jnp.int32, (width, 1), 0).astype(F32)
    ramp = (line + 0.5) / width
    phase = kappa * speeds[0] * line
    cosine, sine = jnp.cos(phase), jnp.sin(phase)
    wave_out[0], wave_out[1] = (1.0 - ramp) * cosine, ramp * cosine
    wave_out[2], wave_out[3] = (1.0 - ramp) * sine, ramp * sine


def second_kernel(
    wave, own, mine_in, other_in, spectrum, along, coupling, qh, ql, rows, lam_col, hats, invs, diags, end_rows, mode, waves, field,
    *, width, modes, nb
):
    count = 2 * mine_in.shape[0]
    kappa = KAPPA_UNIT * wave[...].astype(F32)
    unknowns = 8 * modes
    half = 2 * modes
    lane = lanes((1, 4 * modes))
    inv_split = (invs[0], invs[1]), (invs[2], invs[3])
    sign = parity(width)
    q0, q1 = rows[0:1], rows[1:2]
    robin_weight = q0, kappa * (q0 - q1)
    same, opposite, same_robin, opposite_robin = ((diags[2 * k : 2 * k + 1], diags[2 * k + 1 : 2 * k + 2]) for k in range(4))
    across_hat = hats[0, : 2 * half], hats[1, : 2 * half]
    along_hat = hats[0, 2 * half :], hats[1, 2 * half :]
    tables = {"t": along_hat, "b": along_hat, "l": across_hat, "r": across_hat}
    mode_split = mode[0], mode[1]
    ends = {}
    for k, side in enumerate("tblr"):
        e = [end_rows[4 * k + j : 4 * k + j + 1] for j in range(4)]
        ends[side] = (e[0], e[1]), (e[2], e[3])
    facing = {"t": "b", "b": "t", "l": "r", "r": "l"}

    def spread(proj, side):
        low = lane < half
        if side in "tb":
            real = jnp.where(low, proj, pltpu.roll(proj, half, 1))
            imag = jnp.where(low, pltpu.roll(proj, half, 1), proj)
        else:
            by1, by2, by3 = (pltpu.roll(proj, k * modes, 1) for k in (1, 2, 3))
            block = lane // modes
            real = jnp.where(block == 0, proj, jnp.where(block == 3, by2, by1))
            imag = jnp.where(block == 0, by2, jnp.where(block == 3, proj, by3))
        parts = cmul((real, imag), ends[facing[side]][0])
        return jnp.concatenate(parts, 1)

    def outgoing(c, side):
        z = cmul((c[:, : unknowns // 2], c[:, unknowns // 2 :]), ends[side][1])
        low = lane < half
        if side in "tb":
            z = [a + pltpu.roll(a, half, 1) for a in z]
            z = jnp.where(low, z[0], z[1])
        else:
            z = [a + pltpu.roll(a, 3 * modes, 1) for a in z]
            block = lane // modes
            back = pltpu.roll(z[0], 3 * modes, 1)
            ahead = pltpu.roll(z[1], modes, 1)
            z = jnp.where(
                block == 0, z[0], jnp.where(block == 1, back, jnp.where(block == 2, pltpu.roll(z[1], 2 * modes, 1), ahead))
            )
        return z

    def synth(zs, table):
        size = zs[0].shape[0]
        stacked = jnp.concatenate([a for z in zs for a in (z, -turn(z, half))], 0)
        out = dot(stacked, table)
        return [(out[2 * k * size : (2 * k + 1) * size], out[(2 * k + 1) * size : (2 * k + 2) * size]) for k in range(len(zs))]

    def coarse_of(projs):
        total = 0.0
        for k, side in enumerate("tblr"):
            total = total + dot(coupling[k], spread(projs[side], side))
        return dot(total, mode_split, NT)

    def robin_of(c, base):
        tb = synth([outgoing(c, "t"), outgoing(c, "b")], along_hat)
        lr = synth([outgoing(c, "l"), outgoing(c, "r")], across_hat)
        return {side: add(base[side], s) for side, s in zip("tblr", tb + lr)}

    row = lax.broadcasted_iota(jnp.int32, (count, 1), 0)
    first, last = row % nb == 0, row % nb == nb - 1

    def incoming(out):
        zero = jnp.zeros((nb, width), F32)
        down = lambda a: jnp.concatenate([zero, a[:-nb]], 0)
        up = lambda a: jnp.concatenate([a[nb:], zero], 0)
        right = lambda a: jnp.where(first, 0.0, pltpu.roll(a, 1, 0))
        left = lambda a: jnp.where(last, 0.0, pltpu.roll(a, count - 1, 0))
        move = lambda f, z: (f(z[0]), f(z[1]))
        return {"t": move(down, out["b"]), "b": move(up, out["t"]), "l": move(right, out["r"]), "r": move(left, out["l"])}

    def apply_inverse(vectors):
        size = vectors[0][0].shape[0]
        k = len(vectors)
        stacked = split(jnp.concatenate([v[0] for v in vectors] + [v[1] for v in vectors], 0))
        a, b = dot(stacked, inv_split[0]), dot(stacked, inv_split[1])
        real, imag = a[: k * size] - b[k * size :], a[k * size :] + b[: k * size]
        return [(real[j * size : (j + 1) * size], imag[j * size : (j + 1) * size]) for j in range(k)]

    def scale(r, z):
        return r * z[0], r * z[1]

    def responses(g):
        edge, rob = {}, {}
        for (a, b), (c, d) in ((("t", "b"), ("l", "r")), (("l", "r"), ("t", "b"))):
            vectors = []
            for src in (a, b):
                plain, heavy = scale(q0, g[src]), cmul(g[src], robin_weight)
                vectors += [plain, scale(sign, plain), heavy, scale(sign, heavy)]
            x = apply_inverse(vectors)
            cross = [scale(q0, add(x[k], scale(sign, x[k + 4]))) for k in range(4)]
            edge[c], edge[d], rob[c], rob[d] = cross
        for a, b in (("t", "b"), ("l", "r")):
            edge[a] = add(edge[a], cmul(g[a], same), cmul(g[b], opposite))
            edge[b] = add(edge[b], cmul(g[b], same), cmul(g[a], opposite))
            rob[a] = add(rob[a], cmul(g[a], same_robin), cmul(g[b], opposite_robin))
            rob[b] = add(rob[b], cmul(g[b], same_robin), cmul(g[a], opposite_robin))
        return edge, rob

    mine_rows, other_rows = (r[...].reshape(count // 2, r.shape[2]) for r in (mine_in, other_in))
    odd = own[0] // nb % 2 == 1
    low_rows, high_rows = jnp.where(odd, other_rows, mine_rows), jnp.where(odd, mine_rows, other_rows)
    values = jnp.concatenate([r[k : k + nb] for k in range(0, count // 2, nb) for r in (low_rows, high_rows)], 0)
    lanes_of = 4 * modes
    proj0 = {s: values[:, k * lanes_of : (k + 1) * lanes_of] for k, s in enumerate("tblr")}
    at = 4 * lanes_of
    robin0 = {}
    for s in "tblr":
        robin0[s] = values[:, at : at + width], values[:, at + width : at + 2 * width]
        at += 2 * width

    out1 = robin_of(coarse_of(proj0), robin0)
    edge, rob = responses(incoming(out1))
    proj1 = {}
    for a, b in (("t", "b"), ("l", "r")):
        ja, jb = sub(edge[a], out1[a]), sub(edge[b], out1[b])
        both = contract((jnp.concatenate([ja[0], jb[0]], 0), jnp.concatenate([ja[1], jb[1]], 0)), tables[a])
        proj1[a], proj1[b] = proj0[a] + both[:count], proj0[b] + both[count:]
    base = {s: add(robin0[s], rob[s]) for s in "tblr"}
    out2 = robin_of(coarse_of(proj1), base)
    g2 = incoming(out2)

    mine = own[0]
    picks = [coupling[k, pl.ds(mine, 1), :] for k in range(4)]
    one = (lanes((1, count)) == mine).astype(F32)
    weights = split(jnp.concatenate(picks + [one] * 4, 0))
    mixed = {s: (dot(weights, g2[s][0]), dot(weights, g2[s][1])) for s in "tblr"}
    sent = {s: (dot(weights, out2[s][0]), dot(weights, out2[s][1])) for s in "tblr"}
    base0 = {s: dot(weights, proj0[s]) for s in "tblr"}
    index = {"t": 0, "b": 1, "l": 2, "r": 3}
    rowof = lambda z, k: (z[0][k : k + 1], z[1][k : k + 1])
    vectors = []
    order = []
    for o in "tblr":
        weight = scale(sign, (q0, q0)) if o in "br" else (q0, q0)
        for src in ("lr" if o in "tb" else "tb"):
            z = rowof(mixed[src], index[o])
            vectors.append((weight[0] * z[0], weight[0] * z[1]))
            order.append((o, src))
    x = apply_inverse(vectors)
    total = jnp.zeros((1, unknowns), F32)
    jumps = {}
    for o in "tblr":
        k = 2 * index[o]
        e = scale(q0, add(x[k], scale(sign, x[k + 1])))
        e = add(e, cmul(rowof(mixed[o], index[o]), same), cmul(rowof(mixed[facing[o]], index[o]), opposite))
        jumps[o] = sub(e, rowof(sent[o], index[o]))
    for a, b in (("t", "b"), ("l", "r")):
        rr = jnp.concatenate([jumps[a][0], jumps[b][0]] + [jumps[a][0]] * 6, 0)
        ri = jnp.concatenate([jumps[a][1], jumps[b][1]] + [jumps[a][1]] * 6, 0)
        both = contract((rr, ri), tables[a])
        for j, o in enumerate((a, b)):
            k = index[o]
            total = total + spread(base0[o][k : k + 1] + both[j : j + 1], o)
    c2 = dot(jnp.broadcast_to(total, (8, unknowns)), mode_split, NT)[0:1]

    mine_g = {s: rowof(mixed[s], 4) for s in "tblr"}
    basis = (qh[...], ql[...])
    coeff = []
    zero = jnp.zeros((4, width), F32)
    sq0 = sign * q0
    for part in range(2):
        left_rows = jnp.concatenate([q0, sq0, mine_g["l"][part], mine_g["r"][part], zero], 0)
        right_rows = jnp.concatenate([mine_g["t"][part], mine_g["b"][part], q0, sq0, zero], 0)
        coeff.append(spectrum[part] + dot(left_rows, right_rows, TN))
    coeff = cmul(coeff, inverse_symbol(lam_col[...], rows[4:5], kappa))
    half_way = [dot(basis, coeff[0]), dot(basis, coeff[1])]

    cr, ci = c2[:, : 4 * modes], c2[:, 4 * modes :]
    low = lane < half
    flip = lambda a: pltpu.roll(a, half, 1)
    a0, a1 = jnp.where(low, cr, flip(ci)), jnp.where(low, flip(cr), ci)
    v = waves[0] * a0 + waves[1] * a1 + waves[2] * turn(a0, half) + waves[3] * turn(a1, half)
    along_split = split(along[...])
    field[0] = dot(half_way[0], basis) + dot(v, along_split)
    field[1] = dot(half_way[1], basis) + dot(-turn(v, half), along_split)


def local(forcing, wave_index, directions, row_coupling, col_coupling, mode_coupling):
    width = forcing.shape[1]
    modes = directions.shape[0]
    na, nb = row_coupling.shape[0], col_coupling.shape[0]
    count = na * nb
    size = 4 * 4 * modes + 4 * 2 * width
    basis, values = sine_table(width)
    qh = basis.astype(jnp.bfloat16)
    ql = (basis - qh.astype(np.float32)).astype(jnp.bfloat16)
    sign = 1.0 - 2.0 * (np.arange(width) % 2)
    rows = np.zeros((8, width), np.float32)
    rows[0], rows[1], rows[2], rows[3], rows[4] = basis[0], basis[1], sign * basis[0], sign * basis[1], values
    lam_col = np.ascontiguousarray(values[:, None])
    wave, dirs = wave_index.reshape(1, 1), directions.reshape(1, modes)

    scale = 1.0 / math.sqrt(width) / math.sqrt(modes)
    rc, cc = row_coupling * scale, col_coupling
    pad = lambda m, lo: jnp.pad(m[:, :-1] if lo else m[:, 1:], ((0, 0), (1, 0) if lo else (0, 1)))
    kron = lambda a, b: (a[:, None, :, None] * b[None, :, None, :]).reshape(count, count)
    coupling = jnp.stack([kron(pad(rc, True), cc), kron(pad(rc, False), cc), kron(rc, pad(cc, True)), kron(rc, pad(cc, False))])
    own = (lax.axis_index("row") * nb + lax.axis_index("col")).reshape(1)

    fits = count <= 64
    params = lambda mib: pltpu.CompilerParams(vmem_limit_bytes=mib << 20) if fits else None
    payload, spectrum, hat, along = pl.pallas_call(
        functools.partial(first_kernel, width=width, modes=modes, count=count),
        out_shape=[
            jax.ShapeDtypeStruct((count // 2, 1, size), F32),
            jax.ShapeDtypeStruct((2, width, width), F32),
            jax.ShapeDtypeStruct((2, 8 * modes, width), BF16),
            jax.ShapeDtypeStruct((4 * modes, width), F32),
        ],
        in_specs=[HBM] * 7,
        out_specs=[HBM] * 4,
        scratch_shapes=[
            pltpu.VMEM((1, 1), jnp.int32),
            pltpu.VMEM((1, modes), jnp.int32),
            pltpu.VMEM((2, width, width), F32),
            pltpu.VMEM((width, width), BF16),
            pltpu.VMEM((width, width), BF16),
            pltpu.VMEM((8, width), F32),
            pltpu.VMEM((width, 1), F32),
            pltpu.VMEM((count // 2, 1, size), F32),
            pltpu.VMEM((2, width, width), F32),
            pltpu.VMEM((2, 8 * modes, width), BF16),
            pltpu.VMEM((4 * modes, width), F32),
            pltpu.SemaphoreType.DMA((7,)),
            pltpu.SemaphoreType.DMA((4,)),
        ],
        name="spectrum",
    )(wave, dirs, forcing, qh, ql, rows, lam_col)
    groups = [[a * nb + b for a in range(k, na, 2) for b in range(nb)] for k in range(2)]
    mine = lax.all_to_all(payload, ("row", "col"), 0, 0, axis_index_groups=groups, tiled=True)
    unknowns = mode_coupling.shape[0]
    made = pl.pallas_call(
        functools.partial(table_kernel, width=width, modes=modes),
        out_shape=[
            jax.ShapeDtypeStruct((4, width, width), BF16),
            jax.ShapeDtypeStruct((8, width), F32),
            jax.ShapeDtypeStruct((16, 4 * modes), F32),
            jax.ShapeDtypeStruct((2, unknowns, unknowns), BF16),
            jax.ShapeDtypeStruct((4, width, 4 * modes), F32),
        ],
        in_specs=[VMEM] * 5,
        out_specs=[VMEM] * 5,
        compiler_params=params(12),
        cost_estimate=pl.CostEstimate(flops=1 << 30, bytes_accessed=1 << 21, transcendentals=1 << 18),
        name="tables",
    )(wave, mode_coupling, rows, lam_col, dirs)
    mine, made, coupling = lax.optimization_barrier((mine, made, coupling))
    other = lax.ppermute(mine, "row", [(a, a ^ 1) for a in range(na)])
    return pl.pallas_call(
        functools.partial(second_kernel, width=width, modes=modes, nb=nb),
        out_shape=jax.ShapeDtypeStruct((2, width, width), F32),
        in_specs=[VMEM, SMEM] + [VMEM] * 15,
        out_specs=VMEM,
        compiler_params=params(28),
        name="sweeps",
    )(wave, own, mine, other, spectrum, along, coupling, qh, ql, rows, lam_col, hat, *made)


def solution(mesh):
    return jax.shard_map(
        local,
        mesh=mesh,
        in_specs=(P(None, "row", "col"), P(), P(), P(), P(), P()),
        out_specs=P(None, "row", "col"),
        check_vma=False,
    )
```

```python
import functools
import math

import jax
import jax.numpy as jnp
import numpy as np
from jax import lax
from jax.experimental import pallas as pl
from jax.experimental.pallas import tpu as pltpu
from jax.sharding import PartitionSpec as P

ANGLES = 64
KAPPA_UNIT = 0.04
DAMPING = 0.5
F32 = jnp.float32
BF16 = jnp.bfloat16
NN = (((1,), (0,)), ((), ()))
NT = (((1,), (1,)), ((), ()))
TN = (((0,), (0,)), ((), ()))
VMEM = pl.BlockSpec(memory_space=pltpu.VMEM)
HBM = pl.BlockSpec(memory_space=pltpu.HBM)
SMEM = pl.BlockSpec(memory_space=pltpu.SMEM)


def split(a):
    if isinstance(a, tuple):
        return a
    high = a.astype(BF16)
    return high, (a - high.astype(F32)).astype(BF16)


def dot(a, b, dims=NN):
    ah, al = split(a)
    bh, bl = split(b)
    mul = functools.partial(lax.dot_general, dimension_numbers=dims, preferred_element_type=F32)
    (da,), (db,) = dims[0]
    size = ah.shape[1 - da]
    if size <= 256 and da == 1 and size % 8 == 0:
        both = mul(jnp.concatenate([ah.astype(F32), al.astype(F32)], 0).astype(BF16), bh)
        return both[:size] + (both[size:] + mul(ah, bl))
    if ah.shape[da] % 128 == 0:
        return mul(jnp.concatenate([ah, al, ah], da), jnp.concatenate([bh, bh, bl], db))
    return mul(ah, bh) + (mul(ah, bl) + mul(al, bh))


def cmul(a, b):
    return a[0] * b[0] - a[1] * b[1], a[0] * b[1] + a[1] * b[0]


def add(*terms):
    return sum(t[0] for t in terms[1:]) + terms[0][0], sum(t[1] for t in terms[1:]) + terms[0][1]


def sub(a, b):
    return a[0] - b[0], a[1] - b[1]


def sine_table(width):
    index = np.arange(1, width + 1)
    basis = np.sqrt(2.0 / (width + 1)) * np.sin(np.pi / (width + 1) * (np.outer(index, index) % (2 * width + 2)))
    values = 2.0 - 2.0 * np.cos(np.pi / (width + 1) * index)
    return basis.astype(np.float32), values.astype(np.float32)


def lanes(shape):
    return lax.broadcasted_iota(jnp.int32, shape, len(shape) - 1)


def parity(width):
    return (1 - 2 * (lanes((1, width)) & 1)).astype(F32)


def inverse_symbol(col_values, row_values, kappa):
    shift = kappa * kappa
    real = col_values + row_values - shift
    imag = DAMPING * shift
    norm = 1.0 / (real * real + imag * imag)
    return real * norm, imag * norm


def turn(z, half):
    sign = jnp.where(lanes((1, 2 * half)) < half, -1.0, 1.0)
    return sign * pltpu.roll(z, half, 1)


def contract(rows, table):
    count, half = rows[0].shape[0], table[0].shape[0] // 2
    out = dot(jnp.concatenate(rows, 0), table, NT)
    return out[:count] + turn(out[count:], half)


def turn_column(dirs, modes):
    shape = (modes, modes)
    spot = lax.broadcasted_iota(jnp.int32, shape, 0) == lanes(shape)
    column = jnp.sum(jnp.where(spot, jnp.broadcast_to(dirs[...].astype(F32), shape), 0.0), 1, keepdims=True)
    return 2.0 * math.pi / ANGLES * column


def turn_row(dirs, modes):
    shape = (modes, 4 * modes)
    spot = (lax.broadcasted_iota(jnp.int32, shape, 0) == lanes(shape) % modes).astype(F32)
    row = lax.dot_general(
        jnp.broadcast_to(dirs[...].astype(F32), (8, modes)).astype(BF16), spot.astype(BF16), NN, preferred_element_type=F32
    )
    return 2.0 * math.pi / ANGLES * row[0:1]


def first_kernel(
    wave_in, dirs_in, forcing_in, qh_in, ql_in, rows_in, lam_in, payload_out, spectrum_out, hat_out, along_out,
    wave, dirs, forcing, qh, ql, rows, lam_col, payload, spectrum, hat, along, arrived, left, *, width, modes, count
):
    sources = wave_in, dirs_in, qh_in, ql_in, forcing_in, rows_in, lam_in
    targets = wave, dirs, qh, ql, forcing, rows, lam_col
    copies = [pltpu.make_async_copy(a, b, arrived.at[k]) for k, (a, b) in enumerate(zip(sources, targets))]
    for copy in copies:
        copy.start()
    for copy in copies[:2]:
        copy.wait()
    kappa = KAPPA_UNIT * wave[...].astype(F32)
    line = lanes((1, width)).astype(F32)
    ramp = (line + 0.5) / width
    windows = (1.0 - ramp, ramp)
    theta = turn_column(dirs, modes)
    tables = []
    for speed in (jnp.cos(theta), jnp.sin(theta)):
        phase = kappa * speed * line
        cosine, sine = jnp.cos(phase), jnp.sin(phase)
        tables += [w * cosine for w in windows] + [-w * sine for w in windows]
    table = jnp.concatenate(tables, 0)
    along[...] = table[4 * modes :]
    sends = [
        pltpu.make_async_copy(a, b, left.at[k])
        for k, (a, b) in enumerate(((along, along_out), (hat, hat_out), (spectrum, spectrum_out), (payload, payload_out)))
    ]
    sends[0].start()
    for copy in copies[2:]:
        copy.wait()
    basis = (qh[...], ql[...])
    hats = split(dot(table, basis))
    hat[0], hat[1] = hats
    sends[1].start()
    across_hat = hats[0][: 4 * modes], hats[1][: 4 * modes]
    along_hat = hats[0][4 * modes :], hats[1][4 * modes :]

    half_way = dot(forcing[...].reshape(2 * width, width), basis)
    coeff = [dot(basis, half_way[:width]), dot(basis, half_way[width:])]
    spectrum[0] = coeff[0]
    spectrum[1] = coeff[1]
    sends[2].start()
    inv = inverse_symbol(lam_col[...], rows[4:5], kappa)
    coeff = [split(c) for c in cmul(coeff, inv)]
    weights = split(rows[...])
    out = []
    vectors = []
    for dims, table_hat in ((NN, along_hat), (NT, across_hat)):
        real, imag = dot(weights, coeff[0], dims), dot(weights, coeff[1], dims)
        edges = []
        for near, inner in ((0, 1), (2, 3)):
            e = real[near : near + 1], imag[near : near + 1]
            d = sub(e, (real[inner : inner + 1], imag[inner : inner + 1]))
            edges.append(e)
            vectors += [e[0] - kappa * d[1], e[1] + kappa * d[0]]
        rows_r = jnp.concatenate([edges[0][0], edges[1][0]] + [edges[0][0]] * 6, 0)
        rows_i = jnp.concatenate([edges[0][1], edges[1][1]] + [edges[0][1]] * 6, 0)
        proj = contract((rows_r, rows_i), table_hat)
        out += [proj[0:1], proj[1:2]]
    flat = jnp.concatenate(out + vectors, 1)
    payload[...] = jnp.broadcast_to(flat[None], payload.shape)
    sends[3].start()
    for copy in sends:
        copy.wait()


def table_kernel(
    wave, mode, rows, lam_col, dirs, spectrum, qh, ql, inv_out, diag_out, ends_out, mode_out, wave_out, still, *, width, modes
):
    kappa = KAPPA_UNIT * wave[...].astype(F32)
    half = 2 * modes
    inv = inverse_symbol(lam_col[...], rows[4:5], kappa)
    inv_split = split(inv[0]), split(inv[1])
    for part in range(2):
        for k in range(2):
            inv_out[2 * part + k] = inv_split[part][k]
    sign = parity(width)
    q0, q1 = rows[0:1], rows[1:2]
    diag_rows = split(jnp.concatenate([q0 * q0, sign * q0 * q0, q0 * (q0 - q1), sign * q0 * (q0 - q1)] * 2, 0))
    real, imag = dot(diag_rows, inv_split[0]), dot(diag_rows, inv_split[1])
    diag_out[...] = jnp.concatenate(
        [
            real[0:1], imag[0:1], real[1:2], imag[1:2],
            real[0:1] - kappa * imag[2:3], imag[0:1] + kappa * real[2:3],
            real[1:2] - kappa * imag[3:4], imag[1:2] + kappa * real[3:4],
        ],
        0,
    )
    mode_out[0], mode_out[1] = split(mode[...])

    basis = (qh[...], ql[...])
    coeff = cmul((spectrum[0], spectrum[1]), inv)
    for part in range(2):
        still[part] = dot(dot(basis, coeff[part]), basis)

    lane = lanes((1, 4 * modes))
    theta = turn_row(dirs, modes)
    speeds = jnp.cos(theta), jnp.sin(theta)
    pick = lane // half, (lane // modes) % 2

    def wave_at(axis, x):
        ramp = (x + 0.5) / width
        window = jnp.where(pick[axis] == 0, 1.0 - ramp, ramp)
        phase = kappa * speeds[axis] * float(x)
        return window * jnp.cos(phase), -window * jnp.sin(phase)

    ends = []
    for axis, near, inner in ((0, 0, 1), (0, width - 1, width - 2), (1, 0, 1), (1, width - 1, width - 2)):
        e, n = wave_at(axis, near), wave_at(axis, inner)
        er, ei, nr, ni = e[0], -e[1], n[0], -n[1]
        ends += [e[0], e[1], er - kappa * (ei - ni), ei + kappa * (er - nr)]
    ends_out[...] = jnp.concatenate(ends, 0)
    line = lax.broadcasted_iota(jnp.int32, (width, 1), 0).astype(F32)
    phase = kappa * speeds[0] * line
    wave_out[0], wave_out[1] = jnp.cos(phase), jnp.sin(phase)


def side_kernel(rows, hats, invs, diag, along, qh, ql, jump_out, green_out, along_out, *, width, modes):
    half = 2 * modes
    inv_split = (invs[0], invs[1]), (invs[2], invs[3])
    sign = parity(width)
    q0 = rows[0:1]
    basis = (qh[...].astype(F32) + ql[...].astype(F32)) * q0
    pair = split(jnp.concatenate([basis, basis * sign], 0))
    for part in range(2):
        made = dot(pair, inv_split[part])
        green_out[part], green_out[2 + part] = made[:width], made[width:]
    along_out[0], along_out[1] = split(along[...])
    table = hats[0].astype(F32) + hats[1].astype(F32)
    weighted = table * q0
    stacked = split(jnp.concatenate([weighted, weighted * sign], 0))
    br, bi = dot(stacked, inv_split[0]), dot(stacked, inv_split[1])
    for part, (a, b) in enumerate((("l", "tblr"), ("t", "lrtb"))):
        start = 4 * modes * part
        real, imag = slice(start, start + half), slice(start + half, start + 2 * half)
        blocks = {}
        for k, src in enumerate(b[:2]):
            off = 8 * modes * k
            r, i = slice(real.start + off, real.stop + off), slice(imag.start + off, imag.stop + off)
            blocks[src] = (br[r] - bi[i]) * q0, (br[i] + bi[r]) * q0
        for k, src in enumerate(b[2:]):
            blocks[src] = cmul((table[real], table[imag]), (diag[2 * k : 2 * k + 1], diag[2 * k + 1 : 2 * k + 2]))
        for k, src in enumerate("tblr"):
            high, low = split(jnp.concatenate(blocks[src], 0))
            jump_out[0, start : start + 2 * half, k * width : (k + 1) * width] = high
            jump_out[1, start : start + 2 * half, k * width : (k + 1) * width] = low


def second_kernel(
    wave, own, mine_in, other_in, coupling, picks, rows, hats, invs, diags, end_rows, mode, waves, still,
    jump_table, green, along, qh, ql, field, *, width, modes, nb
):
    count = 2 * mine_in.shape[0]
    kappa = KAPPA_UNIT * wave[...].astype(F32)
    unknowns = 8 * modes
    half = 2 * modes
    lane = lanes((1, 4 * modes))
    inv_split = (invs[0], invs[1]), (invs[2], invs[3])
    sign = parity(width)
    q0, q1 = rows[0:1], rows[1:2]
    robin_weight = q0, kappa * (q0 - q1)
    same, opposite, same_robin, opposite_robin = ((diags[2 * k : 2 * k + 1], diags[2 * k + 1 : 2 * k + 2]) for k in range(4))
    across_hat = hats[0, : 2 * half], hats[1, : 2 * half]
    along_hat = hats[0, 2 * half :], hats[1, 2 * half :]
    tables = {"t": along_hat, "b": along_hat, "l": across_hat, "r": across_hat}
    mode_split = mode[0], mode[1]
    ends = {}
    for k, side in enumerate("tblr"):
        e = [end_rows[4 * k + j : 4 * k + j + 1] for j in range(4)]
        ends[side] = (e[0], e[1]), (e[2], e[3])
    facing = {"t": "b", "b": "t", "l": "r", "r": "l"}

    def spread(proj, side):
        low = lane < half
        if side in "tb":
            real = jnp.where(low, proj, pltpu.roll(proj, half, 1))
            imag = jnp.where(low, pltpu.roll(proj, half, 1), proj)
        else:
            by1, by2, by3 = (pltpu.roll(proj, k * modes, 1) for k in (1, 2, 3))
            block = lane // modes
            real = jnp.where(block == 0, proj, jnp.where(block == 3, by2, by1))
            imag = jnp.where(block == 0, by2, jnp.where(block == 3, proj, by3))
        parts = cmul((real, imag), ends[facing[side]][0])
        return jnp.concatenate(parts, 1)

    def outgoing(c, side):
        z = cmul((c[:, : unknowns // 2], c[:, unknowns // 2 :]), ends[side][1])
        low = lane < half
        if side in "tb":
            z = [a + pltpu.roll(a, half, 1) for a in z]
            z = jnp.where(low, z[0], z[1])
        else:
            z = [a + pltpu.roll(a, 3 * modes, 1) for a in z]
            block = lane // modes
            back = pltpu.roll(z[0], 3 * modes, 1)
            ahead = pltpu.roll(z[1], modes, 1)
            z = jnp.where(
                block == 0, z[0], jnp.where(block == 1, back, jnp.where(block == 2, pltpu.roll(z[1], 2 * modes, 1), ahead))
            )
        return z

    def synth(zs, table):
        size = zs[0].shape[0]
        stacked = jnp.concatenate([a for z in zs for a in (z, -turn(z, half))], 0)
        out = dot(stacked, table)
        return [(out[2 * k * size : (2 * k + 1) * size], out[(2 * k + 1) * size : (2 * k + 2) * size]) for k in range(len(zs))]

    def coarse_of(weights, projs):
        total = 0.0
        for k, side in enumerate("tblr"):
            total = total + spread(dot(weights[k], projs[side]), side)
        return dot(total, mode_split, NT)

    def robin_of(c, base):
        tb = synth([outgoing(c, "t"), outgoing(c, "b")], along_hat)
        lr = synth([outgoing(c, "l"), outgoing(c, "r")], across_hat)
        return {side: add(base[side], s) for side, s in zip("tblr", tb + lr)}

    row = lax.broadcasted_iota(jnp.int32, (count, 1), 0)
    first, last = row % nb == 0, row % nb == nb - 1

    def incoming(out):
        zero = jnp.zeros((nb, width), F32)
        down = lambda a: jnp.concatenate([zero, a[:-nb]], 0)
        up = lambda a: jnp.concatenate([a[nb:], zero], 0)
        right = lambda a: jnp.where(first, 0.0, pltpu.roll(a, 1, 0))
        left = lambda a: jnp.where(last, 0.0, pltpu.roll(a, count - 1, 0))
        move = lambda f, z: (f(z[0]), f(z[1]))
        return {"t": move(down, out["b"]), "b": move(up, out["t"]), "l": move(right, out["r"]), "r": move(left, out["l"])}

    def apply_inverse(vectors):
        size = vectors[0][0].shape[0]
        k = len(vectors)
        stacked = split(jnp.concatenate([v[0] for v in vectors] + [v[1] for v in vectors], 0))
        a, b = dot(stacked, inv_split[0]), dot(stacked, inv_split[1])
        real, imag = a[: k * size] - b[k * size :], a[k * size :] + b[: k * size]
        return [(real[j * size : (j + 1) * size], imag[j * size : (j + 1) * size]) for j in range(k)]

    def scale(r, z):
        return r * z[0], r * z[1]

    jump_split = jump_table[0], jump_table[1]

    def project_sources(rows_of):
        flip = lambda z: scale(sign, z)
        kinds = [
            [rows_of("lt", src) for src in "tblr"],
            [flip(rows_of("r", "t")), flip(rows_of("r", "b")), rows_of("r", "r"), rows_of("r", "l")],
            [rows_of("b", "b"), rows_of("b", "t"), flip(rows_of("b", "l")), flip(rows_of("b", "r"))],
        ]
        size = kinds[0][0][0].shape[0]
        stacked = jnp.concatenate([jnp.concatenate([z[part] for z in kind], 1) for part in range(2) for kind in kinds], 0)
        x = dot(stacked, jump_split, NT)
        block = lambda k, at: (
            x[k * size : (k + 1) * size, at : at + 2 * half] + turn(x[(k + 3) * size : (k + 4) * size, at : at + 2 * half], half)
        )
        return {"l": block(0, 0), "t": block(0, 2 * half), "r": block(1, 0), "b": block(2, 2 * half)}

    def project_sent(sent):
        out = {}
        for a, b in (("t", "b"), ("l", "r")):
            size = sent[a][0].shape[0]
            both = contract([jnp.concatenate([sent[a][k], sent[b][k]], 0) for k in range(2)], tables[a])
            out[a], out[b] = both[:size], both[size:]
        return out

    mine_rows, other_rows = (r[...].reshape(count // 2, r.shape[2]) for r in (mine_in, other_in))
    odd = own[0] // nb % 2 == 1
    low_rows, high_rows = jnp.where(odd, other_rows, mine_rows), jnp.where(odd, mine_rows, other_rows)
    values = jnp.concatenate([r[k : k + nb] for k in range(0, count // 2, nb) for r in (low_rows, high_rows)], 0)
    lanes_of = 4 * modes
    proj0 = {s: values[:, k * lanes_of : (k + 1) * lanes_of] for k, s in enumerate("tblr")}
    at = 4 * lanes_of
    robin0 = {}
    for s in "tblr":
        robin0[s] = values[:, at : at + width], values[:, at + width : at + 2 * width]
        at += 2 * width

    couplings = [split(coupling[k]) for k in range(4)]
    out1 = robin_of(coarse_of(couplings, proj0), robin0)
    g1 = incoming(out1)
    share, sent = project_sources(lambda o, src: g1[src]), project_sent(out1)
    proj1 = {s: proj0[s] + share[s] - sent[s] for s in "tblr"}
    pick = [split(picks[k]) for k in range(4)]
    base = {s: (dot(pick[k], robin0[s][0]), dot(pick[k], robin0[s][1])) for k, s in enumerate("tblr")}
    base_proj = {s: dot(pick[k], proj0[s]) for k, s in enumerate("tblr")}
    every = jnp.concatenate([picks[k] for k in range(4)], 0)
    every_split = split(every)
    mixed1 = {s: (dot(every_split, g1[s][0]), dot(every_split, g1[s][1])) for s in "tblr"}
    group = lambda z, k: (z[0][8 * k : 8 * k + 8], z[1][8 * k : 8 * k + 8])
    vectors = []
    for k, s in enumerate("tblr"):
        for src in "lr" if s in "tb" else "tb":
            z = cmul(group(mixed1[src], k), robin_weight)
            vectors.append(scale(sign, z) if s in "br" else z)
    x = apply_inverse(vectors)
    for k, s in enumerate("tblr"):
        cross = scale(q0, add(x[2 * k], scale(sign, x[2 * k + 1])))
        near, far = group(mixed1[s], k), group(mixed1[facing[s]], k)
        base[s] = add(base[s], cross, cmul(near, same_robin), cmul(far, opposite_robin))
    c1 = coarse_of([split(dot(every_split, couplings[k])) for k in range(4)], proj1)
    tb = synth([outgoing(c1[8 * k : 8 * k + 8], s) for k, s in ((0, "t"), (1, "b"))], along_hat)
    lr = synth([outgoing(c1[8 * k : 8 * k + 8], s) for k, s in ((2, "l"), (3, "r"))], across_hat)
    out2 = {s: add(base[s], z) for s, z in zip("tblr", tb + lr)}

    index = {"t": 0, "b": 1, "l": 2, "r": 3}
    rowof = lambda z, k: (z[0][k : k + 1], z[1][k : k + 1])

    share, sent = project_sources(lambda o, src: out2[facing[src]]), project_sent(out2)
    total = jnp.zeros((1, unknowns), F32)
    for o in "tblr":
        total = total + spread(base_proj[o][5:6] + share[o][index[o] : index[o] + 1] - sent[o][5:6], o)
    c2 = dot(jnp.broadcast_to(total, (8, unknowns)), mode_split, NT)[0:1]

    mine_g = {s: rowof(out2[facing[s]], 4) for s in "tblr"}
    basis = (qh[...], ql[...])
    near, far = (green[0], green[1]), (green[2], green[3])
    across_rows = add(cmul(near, mine_g["t"]), cmul(far, mine_g["b"]))
    across_cols = add(cmul(near, mine_g["l"]), cmul(far, mine_g["r"]))
    solved = [still[k] + dot(across_rows[k], basis) + dot(basis, across_cols[k], NT) for k in range(2)]

    cr, ci = c2[:, : 4 * modes], c2[:, 4 * modes :]
    low = lane < half
    flip = lambda a: pltpu.roll(a, half, 1)
    a0, a1 = jnp.where(low, cr, flip(ci)), jnp.where(low, flip(cr), ci)
    ramp = (lax.broadcasted_iota(jnp.int32, (width, 1), 0).astype(F32) + 0.5) / width
    blend = lambda lo, hi: lo + ramp * (hi - lo)
    v = waves[0] * blend(a0, a1) + waves[1] * blend(turn(a0, half), turn(a1, half))
    along_split = along[0], along[1]
    field[0] = solved[0] + dot(v, along_split)
    field[1] = solved[1] + dot(-turn(v, half), along_split)


def local(forcing, wave_index, directions, row_coupling, col_coupling, mode_coupling):
    width = forcing.shape[1]
    modes = directions.shape[0]
    na, nb = row_coupling.shape[0], col_coupling.shape[0]
    count = na * nb
    size = 4 * 4 * modes + 4 * 2 * width
    basis, values = sine_table(width)
    qh = basis.astype(jnp.bfloat16)
    ql = (basis - qh.astype(np.float32)).astype(jnp.bfloat16)
    sign = 1.0 - 2.0 * (np.arange(width) % 2)
    rows = np.zeros((8, width), np.float32)
    rows[0], rows[1], rows[2], rows[3], rows[4] = basis[0], basis[1], sign * basis[0], sign * basis[1], values
    lam_col = np.ascontiguousarray(values[:, None])
    wave, dirs = wave_index.reshape(1, 1), directions.reshape(1, modes)

    scale = 1.0 / math.sqrt(width) / math.sqrt(modes)
    rc, cc = row_coupling * scale, col_coupling
    pad = lambda m, lo: jnp.pad(m[:, :-1] if lo else m[:, 1:], ((0, 0), (1, 0) if lo else (0, 1)))
    kron = lambda a, b: (a[:, None, :, None] * b[None, :, None, :]).reshape(count, count)
    coupling = jnp.stack([kron(pad(rc, True), cc), kron(pad(rc, False), cc), kron(rc, pad(cc, True)), kron(rc, pad(cc, False))])
    own = (lax.axis_index("row") * nb + lax.axis_index("col")).reshape(1)
    tile = jnp.arange(count)
    taken = lax.dynamic_slice_in_dim(coupling, own[0], 1, 1)[:, 0]
    sums = jnp.concatenate([taken, (tile == own[0]).astype(F32)[None]])
    ahead = lambda m, by: jnp.pad(m[:, by:], ((0, 0), (0, by)))
    behind = lambda m, by: jnp.pad(m[:, :-by], ((0, 0), (by, 0)))
    moved = jnp.stack(
        [
            behind(sums, nb),
            ahead(sums, nb),
            jnp.where(tile % nb == 0, 0.0, behind(sums, 1)),
            jnp.where(tile % nb == nb - 1, 0.0, ahead(sums, 1)),
        ]
    )
    picks = jnp.concatenate([moved, taken[:, None], jnp.zeros((4, 2, count), F32)], 1)

    fits = count <= 64
    params = lambda mib: pltpu.CompilerParams(vmem_limit_bytes=mib << 20) if fits else None
    payload, spectrum, hat, along = pl.pallas_call(
        functools.partial(first_kernel, width=width, modes=modes, count=count),
        out_shape=[
            jax.ShapeDtypeStruct((count // 2, 1, size), F32),
            jax.ShapeDtypeStruct((2, width, width), F32),
            jax.ShapeDtypeStruct((2, 8 * modes, width), BF16),
            jax.ShapeDtypeStruct((4 * modes, width), F32),
        ],
        in_specs=[HBM] * 7,
        out_specs=[HBM] * 4,
        scratch_shapes=[
            pltpu.VMEM((1, 1), jnp.int32),
            pltpu.VMEM((1, modes), jnp.int32),
            pltpu.VMEM((2, width, width), F32),
            pltpu.VMEM((width, width), BF16),
            pltpu.VMEM((width, width), BF16),
            pltpu.VMEM((8, width), F32),
            pltpu.VMEM((width, 1), F32),
            pltpu.VMEM((count // 2, 1, size), F32),
            pltpu.VMEM((2, width, width), F32),
            pltpu.VMEM((2, 8 * modes, width), BF16),
            pltpu.VMEM((4 * modes, width), F32),
            pltpu.SemaphoreType.DMA((7,)),
            pltpu.SemaphoreType.DMA((4,)),
        ],
        name="spectrum",
    )(wave, dirs, forcing, qh, ql, rows, lam_col)
    groups = [[a * nb + b for a in range(k, na, 2) for b in range(nb)] for k in range(2)]
    mine = lax.all_to_all(payload, ("row", "col"), 0, 0, axis_index_groups=groups, tiled=True)
    unknowns = mode_coupling.shape[0]
    estimate = pl.CostEstimate(flops=1 << 30, bytes_accessed=1 << 21, transcendentals=1 << 18)
    invs, diags, ends, mode, waves, still = pl.pallas_call(
        functools.partial(table_kernel, width=width, modes=modes),
        out_shape=[
            jax.ShapeDtypeStruct((4, width, width), BF16),
            jax.ShapeDtypeStruct((8, width), F32),
            jax.ShapeDtypeStruct((16, 4 * modes), F32),
            jax.ShapeDtypeStruct((2, unknowns, unknowns), BF16),
            jax.ShapeDtypeStruct((2, width, 4 * modes), F32),
            jax.ShapeDtypeStruct((2, width, width), F32),
        ],
        in_specs=[VMEM] * 8,
        out_specs=[VMEM] * 6,
        compiler_params=params(16),
        cost_estimate=estimate,
        name="tables",
    )(wave, mode_coupling, rows, lam_col, dirs, spectrum, qh, ql)
    mine, invs, diags, ends, mode, waves, still, coupling, picks, hat, along = lax.optimization_barrier(
        (mine, invs, diags, ends, mode, waves, still, coupling, picks, hat, along)
    )
    other = lax.ppermute(mine, "row", [(a, a ^ 1) for a in range(na)])
    jumps, green, along = pl.pallas_call(
        functools.partial(side_kernel, width=width, modes=modes),
        out_shape=[
            jax.ShapeDtypeStruct((2, 8 * modes, 4 * width), BF16),
            jax.ShapeDtypeStruct((4, width, width), F32),
            jax.ShapeDtypeStruct((2, 4 * modes, width), BF16),
        ],
        in_specs=[VMEM] * 7,
        out_specs=[VMEM] * 3,
        compiler_params=params(16),
        cost_estimate=estimate,
        name="sides",
    )(rows, hat, invs, diags, along, qh, ql)
    return pl.pallas_call(
        functools.partial(second_kernel, width=width, modes=modes, nb=nb),
        out_shape=jax.ShapeDtypeStruct((2, width, width), F32),
        in_specs=[VMEM, SMEM] + [VMEM] * 17,
        out_specs=VMEM,
        compiler_params=params(28),
        name="sweeps",
    )(wave, own, mine, other, coupling, picks, rows, hat, invs, diags, ends, mode, waves, still, jumps, green, along, qh, ql)


def solution(mesh):
    return jax.shard_map(
        local,
        mesh=mesh,
        in_specs=(P(None, "row", "col"), P(), P(), P(), P(), P()),
        out_specs=P(None, "row", "col"),
        check_vma=False,
    )
```

```python
import functools
import math

import jax
import jax.numpy as jnp
import numpy as np
from jax import lax
from jax.experimental import pallas as pl
from jax.experimental.pallas import tpu as pltpu
from jax.sharding import PartitionSpec as P

ANGLES = 64
KAPPA_UNIT = 0.04
DAMPING = 0.5
F32 = jnp.float32
BF16 = jnp.bfloat16
NN = (((1,), (0,)), ((), ()))
NT = (((1,), (1,)), ((), ()))
TN = (((0,), (0,)), ((), ()))
VMEM = pl.BlockSpec(memory_space=pltpu.VMEM)
HBM = pl.BlockSpec(memory_space=pltpu.HBM)
SMEM = pl.BlockSpec(memory_space=pltpu.SMEM)


def split(a):
    if isinstance(a, tuple):
        return a
    high = a.astype(BF16)
    return high, (a - high.astype(F32)).astype(BF16)


def dot(a, b, dims=NN):
    ah, al = split(a)
    bh, bl = split(b)
    mul = functools.partial(lax.dot_general, dimension_numbers=dims, preferred_element_type=F32)
    (da,), (db,) = dims[0]
    size = ah.shape[1 - da]
    if size <= 256 and da == 1 and size % 8 == 0:
        both = mul(jnp.concatenate([ah.astype(F32), al.astype(F32)], 0).astype(BF16), bh)
        return both[:size] + (both[size:] + mul(ah, bl))
    if ah.shape[da] % 128 == 0:
        return mul(jnp.concatenate([ah, al, ah], da), jnp.concatenate([bh, bh, bl], db))
    return mul(ah, bh) + (mul(ah, bl) + mul(al, bh))


def cmul(a, b):
    return a[0] * b[0] - a[1] * b[1], a[0] * b[1] + a[1] * b[0]


def add(*terms):
    return sum(t[0] for t in terms[1:]) + terms[0][0], sum(t[1] for t in terms[1:]) + terms[0][1]


def sub(a, b):
    return a[0] - b[0], a[1] - b[1]


def sine_table(width):
    index = np.arange(1, width + 1)
    basis = np.sqrt(2.0 / (width + 1)) * np.sin(np.pi / (width + 1) * (np.outer(index, index) % (2 * width + 2)))
    values = 2.0 - 2.0 * np.cos(np.pi / (width + 1) * index)
    return basis.astype(np.float32), values.astype(np.float32)


def lanes(shape):
    return lax.broadcasted_iota(jnp.int32, shape, len(shape) - 1)


def parity(width):
    return (1 - 2 * (lanes((1, width)) & 1)).astype(F32)


def inverse_symbol(col_values, row_values, kappa):
    shift = kappa * kappa
    real = col_values + row_values - shift
    imag = DAMPING * shift
    norm = 1.0 / (real * real + imag * imag)
    return real * norm, imag * norm


def turn(z, half):
    sign = jnp.where(lanes((1, 2 * half)) < half, -1.0, 1.0)
    return sign * pltpu.roll(z, half, 1)


def contract(rows, table, dims=NT):
    count, half = rows[0].shape[0], table[0].shape[1 - dims[0][1][0]] // 2
    out = dot(jnp.concatenate(rows, 0), table, dims)
    return out[:count] + turn(out[count:], half)


def turn_column(dirs, modes):
    shape = (modes, modes)
    spot = lax.broadcasted_iota(jnp.int32, shape, 0) == lanes(shape)
    column = jnp.sum(jnp.where(spot, jnp.broadcast_to(dirs[...].astype(F32), shape), 0.0), 1, keepdims=True)
    return 2.0 * math.pi / ANGLES * column


def turn_row(dirs, modes):
    shape = (modes, 4 * modes)
    spot = (lax.broadcasted_iota(jnp.int32, shape, 0) == lanes(shape) % modes).astype(F32)
    row = lax.dot_general(
        jnp.broadcast_to(dirs[...].astype(F32), (8, modes)).astype(BF16), spot.astype(BF16), NN, preferred_element_type=F32
    )
    return 2.0 * math.pi / ANGLES * row[0:1]


def wave_table(kappa, theta, width):
    line = lanes((1, width)).astype(F32)
    ramp = (line + 0.5) / width
    windows = (1.0 - ramp, ramp)
    tables = []
    for speed in (jnp.cos(theta), jnp.sin(theta)):
        phase = kappa * speed * line
        cosine, sine = jnp.cos(phase), jnp.sin(phase)
        tables += [w * cosine for w in windows] + [-w * sine for w in windows]
    return jnp.concatenate(tables, 0)


def first_kernel(
    wave_in, dirs_in, forcing_in, qh_in, ql_in, rows_in, lam_in, payload,
    wave, dirs, forcing, qh, ql, rows, lam_col, arrived, *, width, modes
):
    sources = wave_in, dirs_in, qh_in, ql_in, forcing_in, rows_in, lam_in
    targets = wave, dirs, qh, ql, forcing, rows, lam_col
    copies = [pltpu.make_async_copy(a, b, arrived.at[k]) for k, (a, b) in enumerate(zip(sources, targets))]
    for copy in copies:
        copy.start()
    for copy in copies[:2]:
        copy.wait()
    kappa = KAPPA_UNIT * wave[...].astype(F32)
    table = wave_table(kappa, turn_column(dirs, modes), width)
    for copy in copies[2:]:
        copy.wait()
    basis = (qh[...], ql[...])
    hats = split(dot(table, basis))
    across_hat = hats[0][: 4 * modes], hats[1][: 4 * modes]
    along_hat = hats[0][4 * modes :], hats[1][4 * modes :]

    half_way = dot(forcing[...].reshape(2 * width, width), basis)
    coeff = [dot(basis, half_way[:width]), dot(basis, half_way[width:])]
    inv = inverse_symbol(lam_col[...], rows[4:5], kappa)
    coeff = [split(c) for c in cmul(coeff, inv)]
    weights = split(rows[...])
    out = []
    vectors = []
    for dims, table_hat in ((NN, along_hat), (NT, across_hat)):
        real, imag = dot(weights, coeff[0], dims), dot(weights, coeff[1], dims)
        edges = []
        for near, inner in ((0, 1), (2, 3)):
            e = real[near : near + 1], imag[near : near + 1]
            d = sub(e, (real[inner : inner + 1], imag[inner : inner + 1]))
            edges.append(e)
            vectors += [e[0] - kappa * d[1], e[1] + kappa * d[0]]
        rows_r = jnp.concatenate([edges[0][0], edges[1][0]] + [edges[0][0]] * 6, 0)
        rows_i = jnp.concatenate([edges[0][1], edges[1][1]] + [edges[0][1]] * 6, 0)
        proj = contract((rows_r, rows_i), table_hat)
        out += [proj[0:1], proj[1:2]]
    flat = jnp.concatenate(out + vectors, 1)
    payload[...] = jnp.broadcast_to(flat[None], payload.shape)


def table_kernel(
    wave, mode, rows, lam_col, dirs, forcing, qh, ql,
    inv_out, diag_out, ends_out, mode_out, wave_out, still, hat_out, along_out, *, width, modes
):
    kappa = KAPPA_UNIT * wave[...].astype(F32)
    half = 2 * modes
    inv = inverse_symbol(lam_col[...], rows[4:5], kappa)
    inv_split = split(inv[0]), split(inv[1])
    for part in range(2):
        for k in range(2):
            inv_out[2 * part + k] = inv_split[part][k]
    sign = parity(width)
    q0, q1 = rows[0:1], rows[1:2]
    diag_rows = split(jnp.concatenate([q0 * q0, sign * q0 * q0, q0 * (q0 - q1), sign * q0 * (q0 - q1)] * 2, 0))
    real, imag = dot(diag_rows, inv_split[0]), dot(diag_rows, inv_split[1])
    diag_out[...] = jnp.concatenate(
        [
            real[0:1], imag[0:1], real[1:2], imag[1:2],
            real[0:1] - kappa * imag[2:3], imag[0:1] + kappa * real[2:3],
            real[1:2] - kappa * imag[3:4], imag[1:2] + kappa * real[3:4],
        ],
        0,
    )
    mode_out[0], mode_out[1] = split(mode[...])

    basis = (qh[...], ql[...])
    half_way = dot(forcing[...].reshape(2 * width, width), basis)
    coeff = cmul((dot(basis, half_way[:width]), dot(basis, half_way[width:])), inv)
    for part in range(2):
        still[part] = dot(dot(basis, coeff[part]), basis)
    table = wave_table(kappa, turn_column(dirs, modes), width)
    along_out[0], along_out[1] = split(table[4 * modes :])
    hat_out[0], hat_out[1] = split(dot(table, basis))

    lane = lanes((1, 4 * modes))
    theta = turn_row(dirs, modes)
    speeds = jnp.cos(theta), jnp.sin(theta)
    pick = lane // half, (lane // modes) % 2

    def wave_at(axis, x):
        ramp = (x + 0.5) / width
        window = jnp.where(pick[axis] == 0, 1.0 - ramp, ramp)
        phase = kappa * speeds[axis] * float(x)
        return window * jnp.cos(phase), -window * jnp.sin(phase)

    ends = []
    for axis, near, inner in ((0, 0, 1), (0, width - 1, width - 2), (1, 0, 1), (1, width - 1, width - 2)):
        e, n = wave_at(axis, near), wave_at(axis, inner)
        er, ei, nr, ni = e[0], -e[1], n[0], -n[1]
        ends += [e[0], e[1], er - kappa * (ei - ni), ei + kappa * (er - nr)]
    ends_out[...] = jnp.concatenate(ends, 0)
    line = lax.broadcasted_iota(jnp.int32, (width, 1), 0).astype(F32)
    phase = kappa * speeds[0] * line
    wave_out[0], wave_out[1] = jnp.cos(phase), jnp.sin(phase)


def side_kernel(rows, cols, hats, invs, diag_rows, qh, ql, jump_out, green_out, turned_out, *, width, modes):
    half = 2 * modes
    inv_split = (invs[0], invs[1]), (invs[2], invs[3])
    sign = parity(width)
    q0 = rows[0:1]
    basis = (qh[...].astype(F32) + ql[...].astype(F32)) * q0
    pair = split(jnp.concatenate([basis, basis * sign], 0))
    for part in range(2):
        made = dot(pair, inv_split[part])
        green_out[part], green_out[2 + part] = made[:width], made[width:]
    table = hats[0].astype(F32) + hats[1].astype(F32)
    turned = table.T
    turned_out[0], turned_out[1] = split(turned)
    weighted = table * q0
    stacked = split(jnp.concatenate([weighted, weighted * sign], 0))
    real, imag = dot(inv_split[0], stacked, NT), dot(inv_split[1], stacked, NT)
    diag = diag_rows[...].T
    size = 2 * half
    for part, sources in enumerate(("tblr", "lrtb")):
        at = slice(size * part, size * part + size)
        blocks = {}
        for k, src in enumerate(sources[:2]):
            off = slice(at.start + 2 * size * k, at.stop + 2 * size * k)
            blocks[src] = (real[:, off] + turn(imag[:, off], half)) * cols[...]
        for k, src in enumerate(sources[2:]):
            blocks[src] = turned[:, at] * diag[:, 2 * k : 2 * k + 1] + turn(turned[:, at], half) * diag[:, 2 * k + 1 : 2 * k + 2]
        for k, src in enumerate("tblr"):
            high, low = split(blocks[src])
            jump_out[0, k * width : (k + 1) * width, at] = high
            jump_out[1, k * width : (k + 1) * width, at] = low


def second_kernel(
    wave, own, mine_in, other_in, coupling, picks, rows, hats, invs, diags, end_rows, mode, waves, still,
    jump_table, green, turned, along, qh, ql, field, *, width, modes, nb
):
    count = 2 * mine_in.shape[0]
    kappa = KAPPA_UNIT * wave[...].astype(F32)
    unknowns = 8 * modes
    half = 2 * modes
    lane = lanes((1, 4 * modes))
    inv_split = (invs[0], invs[1]), (invs[2], invs[3])
    sign = parity(width)
    q0, q1 = rows[0:1], rows[1:2]
    robin_weight = q0, kappa * (q0 - q1)
    same, opposite, same_robin, opposite_robin = ((diags[2 * k : 2 * k + 1], diags[2 * k + 1 : 2 * k + 2]) for k in range(4))
    across_hat = hats[0, : 2 * half], hats[1, : 2 * half]
    along_hat = hats[0, 2 * half :], hats[1, 2 * half :]
    across_turned = turned[0, :, : 2 * half], turned[1, :, : 2 * half]
    along_turned = turned[0, :, 2 * half :], turned[1, :, 2 * half :]
    tables = {"t": along_turned, "l": across_turned}
    mode_split = mode[0], mode[1]
    ends = {}
    for k, side in enumerate("tblr"):
        e = [end_rows[4 * k + j : 4 * k + j + 1] for j in range(4)]
        ends[side] = (e[0], e[1]), (e[2], e[3])
    facing = {"t": "b", "b": "t", "l": "r", "r": "l"}

    def spread(proj, side):
        low = lane < half
        if side in "tb":
            real = jnp.where(low, proj, pltpu.roll(proj, half, 1))
            imag = jnp.where(low, pltpu.roll(proj, half, 1), proj)
        else:
            by1, by2, by3 = (pltpu.roll(proj, k * modes, 1) for k in (1, 2, 3))
            block = lane // modes
            real = jnp.where(block == 0, proj, jnp.where(block == 3, by2, by1))
            imag = jnp.where(block == 0, by2, jnp.where(block == 3, proj, by3))
        parts = cmul((real, imag), ends[facing[side]][0])
        return jnp.concatenate(parts, 1)

    def outgoing(c, side):
        z = cmul((c[:, : unknowns // 2], c[:, unknowns // 2 :]), ends[side][1])
        low = lane < half
        if side in "tb":
            z = [a + pltpu.roll(a, half, 1) for a in z]
            z = jnp.where(low, z[0], z[1])
        else:
            z = [a + pltpu.roll(a, 3 * modes, 1) for a in z]
            block = lane // modes
            back = pltpu.roll(z[0], 3 * modes, 1)
            ahead = pltpu.roll(z[1], modes, 1)
            z = jnp.where(
                block == 0, z[0], jnp.where(block == 1, back, jnp.where(block == 2, pltpu.roll(z[1], 2 * modes, 1), ahead))
            )
        return z

    def synth(zs, table):
        size = zs[0].shape[0]
        stacked = jnp.concatenate([a for z in zs for a in (z, -turn(z, half))], 0)
        out = dot(stacked, table)
        return [(out[2 * k * size : (2 * k + 1) * size], out[(2 * k + 1) * size : (2 * k + 2) * size]) for k in range(len(zs))]

    def coarse_of(weights, projs):
        total = 0.0
        for k, side in enumerate("tblr"):
            total = total + spread(dot(weights[k], projs[side]), side)
        return dot(total, mode_split, NT)

    def robin_of(c, base):
        tb = synth([outgoing(c, "t"), outgoing(c, "b")], along_hat)
        lr = synth([outgoing(c, "l"), outgoing(c, "r")], across_hat)
        return {side: add(base[side], s) for side, s in zip("tblr", tb + lr)}

    row = lax.broadcasted_iota(jnp.int32, (count, 1), 0)
    first, last = row % nb == 0, row % nb == nb - 1

    def incoming(out):
        zero = jnp.zeros((nb, width), F32)
        down = lambda a: jnp.concatenate([zero, a[:-nb]], 0)
        up = lambda a: jnp.concatenate([a[nb:], zero], 0)
        right = lambda a: jnp.where(first, 0.0, pltpu.roll(a, 1, 0))
        left = lambda a: jnp.where(last, 0.0, pltpu.roll(a, count - 1, 0))
        move = lambda f, z: (f(z[0]), f(z[1]))
        return {"t": move(down, out["b"]), "b": move(up, out["t"]), "l": move(right, out["r"]), "r": move(left, out["l"])}

    def apply_inverse(vectors):
        size = vectors[0][0].shape[0]
        k = len(vectors)
        stacked = split(jnp.concatenate([v[0] for v in vectors] + [v[1] for v in vectors], 0))
        a, b = dot(stacked, inv_split[0]), dot(stacked, inv_split[1])
        real, imag = a[: k * size] - b[k * size :], a[k * size :] + b[: k * size]
        return [(real[j * size : (j + 1) * size], imag[j * size : (j + 1) * size]) for j in range(k)]

    def scale(r, z):
        return r * z[0], r * z[1]

    jump_split = jump_table[0], jump_table[1]

    def project_sources(rows_of):
        flip = lambda z: scale(sign, z)
        kinds = [
            [rows_of("lt", src) for src in "tblr"],
            [flip(rows_of("r", "t")), flip(rows_of("r", "b")), rows_of("r", "r"), rows_of("r", "l")],
            [rows_of("b", "b"), rows_of("b", "t"), flip(rows_of("b", "l")), flip(rows_of("b", "r"))],
        ]
        size = kinds[0][0][0].shape[0]
        stacked = jnp.concatenate([jnp.concatenate([z[part] for z in kind], 1) for part in range(2) for kind in kinds], 0)
        x = dot(stacked, jump_split)
        block = lambda k, at: (
            x[k * size : (k + 1) * size, at : at + 2 * half] + turn(x[(k + 3) * size : (k + 4) * size, at : at + 2 * half], half)
        )
        return {"l": block(0, 0), "t": block(0, 2 * half), "r": block(1, 0), "b": block(2, 2 * half)}

    def project_sent(sent):
        out = {}
        for a, b in (("t", "b"), ("l", "r")):
            size = sent[a][0].shape[0]
            both = contract([jnp.concatenate([sent[a][k], sent[b][k]], 0) for k in range(2)], tables[a], NN)
            out[a], out[b] = both[:size], both[size:]
        return out

    mine_rows, other_rows = (r[...].reshape(count // 2, r.shape[2]) for r in (mine_in, other_in))
    odd = own[0] // nb % 2 == 1
    low_rows, high_rows = jnp.where(odd, other_rows, mine_rows), jnp.where(odd, mine_rows, other_rows)
    values = jnp.concatenate([r[k : k + nb] for k in range(0, count // 2, nb) for r in (low_rows, high_rows)], 0)
    lanes_of = 4 * modes
    proj0 = {s: values[:, k * lanes_of : (k + 1) * lanes_of] for k, s in enumerate("tblr")}
    at = 4 * lanes_of
    robin0 = {}
    for s in "tblr":
        robin0[s] = values[:, at : at + width], values[:, at + width : at + 2 * width]
        at += 2 * width

    couplings = [split(coupling[k]) for k in range(4)]
    out1 = robin_of(coarse_of(couplings, proj0), robin0)
    g1 = incoming(out1)
    share, sent = project_sources(lambda o, src: g1[src]), project_sent(out1)
    proj1 = {s: proj0[s] + share[s] - sent[s] for s in "tblr"}
    pick = [split(picks[k]) for k in range(4)]
    base = {s: (dot(pick[k], robin0[s][0]), dot(pick[k], robin0[s][1])) for k, s in enumerate("tblr")}
    base_proj = {s: dot(pick[k], proj0[s]) for k, s in enumerate("tblr")}
    every = jnp.concatenate([picks[k] for k in range(4)], 0)
    every_split = split(every)
    mixed1 = {s: (dot(every_split, g1[s][0]), dot(every_split, g1[s][1])) for s in "tblr"}
    group = lambda z, k: (z[0][8 * k : 8 * k + 8], z[1][8 * k : 8 * k + 8])
    vectors = []
    for k, s in enumerate("tblr"):
        for src in "lr" if s in "tb" else "tb":
            z = cmul(group(mixed1[src], k), robin_weight)
            vectors.append(scale(sign, z) if s in "br" else z)
    x = apply_inverse(vectors)
    for k, s in enumerate("tblr"):
        cross = scale(q0, add(x[2 * k], scale(sign, x[2 * k + 1])))
        near, far = group(mixed1[s], k), group(mixed1[facing[s]], k)
        base[s] = add(base[s], cross, cmul(near, same_robin), cmul(far, opposite_robin))
    c1 = coarse_of([split(dot(every_split, couplings[k])) for k in range(4)], proj1)
    tb = synth([outgoing(c1[8 * k : 8 * k + 8], s) for k, s in ((0, "t"), (1, "b"))], along_hat)
    lr = synth([outgoing(c1[8 * k : 8 * k + 8], s) for k, s in ((2, "l"), (3, "r"))], across_hat)
    out2 = {s: add(base[s], z) for s, z in zip("tblr", tb + lr)}

    index = {"t": 0, "b": 1, "l": 2, "r": 3}
    rowof = lambda z, k: (z[0][k : k + 1], z[1][k : k + 1])

    share, sent = project_sources(lambda o, src: out2[facing[src]]), project_sent(out2)
    total = jnp.zeros((1, unknowns), F32)
    for o in "tblr":
        total = total + spread(base_proj[o][5:6] + share[o][index[o] : index[o] + 1] - sent[o][5:6], o)
    c2 = dot(jnp.broadcast_to(total, (8, unknowns)), mode_split, NT)[0:1]

    mine_g = {s: rowof(out2[facing[s]], 4) for s in "tblr"}
    basis = (qh[...], ql[...])
    near, far = (green[0], green[1]), (green[2], green[3])
    across_rows = add(cmul(near, mine_g["t"]), cmul(far, mine_g["b"]))
    across_cols = add(cmul(near, mine_g["l"]), cmul(far, mine_g["r"]))
    solved = [still[k] + dot(across_rows[k], basis) + dot(basis, across_cols[k], NT) for k in range(2)]

    cr, ci = c2[:, : 4 * modes], c2[:, 4 * modes :]
    low = lane < half
    flip = lambda a: pltpu.roll(a, half, 1)
    a0, a1 = jnp.where(low, cr, flip(ci)), jnp.where(low, flip(cr), ci)
    ramp = (lax.broadcasted_iota(jnp.int32, (width, 1), 0).astype(F32) + 0.5) / width
    blend = lambda lo, hi: lo + ramp * (hi - lo)
    v = waves[0] * blend(a0, a1) + waves[1] * blend(turn(a0, half), turn(a1, half))
    along_split = along[0], along[1]
    field[0] = solved[0] + dot(v, along_split)
    field[1] = solved[1] + dot(-turn(v, half), along_split)


def local(forcing, wave_index, directions, row_coupling, col_coupling, mode_coupling):
    width = forcing.shape[1]
    modes = directions.shape[0]
    na, nb = row_coupling.shape[0], col_coupling.shape[0]
    count = na * nb
    size = 4 * 4 * modes + 4 * 2 * width
    basis, values = sine_table(width)
    qh = basis.astype(jnp.bfloat16)
    ql = (basis - qh.astype(np.float32)).astype(jnp.bfloat16)
    sign = 1.0 - 2.0 * (np.arange(width) % 2)
    rows = np.zeros((8, width), np.float32)
    rows[0], rows[1], rows[2], rows[3], rows[4] = basis[0], basis[1], sign * basis[0], sign * basis[1], values
    lam_col, col = values[:, None], basis[0][:, None]
    wave, dirs = wave_index.reshape(1, 1), directions.reshape(1, modes)

    scale = 1.0 / math.sqrt(width) / math.sqrt(modes)
    rc, cc = row_coupling * scale, col_coupling
    pad = lambda m, lo: jnp.pad(m[:, :-1] if lo else m[:, 1:], ((0, 0), (1, 0) if lo else (0, 1)))
    kron = lambda a, b: (a[:, None, :, None] * b[None, :, None, :]).reshape(count, count)
    coupling = jnp.stack([kron(pad(rc, True), cc), kron(pad(rc, False), cc), kron(rc, pad(cc, True)), kron(rc, pad(cc, False))])
    own = (lax.axis_index("row") * nb + lax.axis_index("col")).reshape(1)
    tile = jnp.arange(count)
    taken = lax.dynamic_slice_in_dim(coupling, own[0], 1, 1)[:, 0]
    sums = jnp.concatenate([taken, (tile == own[0]).astype(F32)[None]])
    ahead = lambda m, by: jnp.pad(m[:, by:], ((0, 0), (0, by)))
    behind = lambda m, by: jnp.pad(m[:, :-by], ((0, 0), (by, 0)))
    moved = jnp.stack(
        [
            behind(sums, nb),
            ahead(sums, nb),
            jnp.where(tile % nb == 0, 0.0, behind(sums, 1)),
            jnp.where(tile % nb == nb - 1, 0.0, ahead(sums, 1)),
        ]
    )
    picks = jnp.concatenate([moved, taken[:, None], jnp.zeros((4, 2, count), F32)], 1)

    fits = count <= 64
    params = lambda mib: pltpu.CompilerParams(vmem_limit_bytes=mib << 20) if fits else None
    payload = pl.pallas_call(
        functools.partial(first_kernel, width=width, modes=modes),
        out_shape=jax.ShapeDtypeStruct((count // 2, 1, size), F32),
        in_specs=[HBM] * 7,
        out_specs=VMEM,
        scratch_shapes=[
            pltpu.VMEM((1, 1), jnp.int32),
            pltpu.VMEM((1, modes), jnp.int32),
            pltpu.VMEM((2, width, width), F32),
            pltpu.VMEM((width, width), BF16),
            pltpu.VMEM((width, width), BF16),
            pltpu.VMEM((8, width), F32),
            pltpu.VMEM((width, 1), F32),
            pltpu.SemaphoreType.DMA((7,)),
        ],
        name="spectrum",
    )(wave, dirs, forcing, qh, ql, rows, lam_col)
    groups = [[a * nb + b for a in range(k, na, 2) for b in range(nb)] for k in range(2)]
    mine = lax.all_to_all(payload, ("row", "col"), 0, 0, axis_index_groups=groups, tiled=True)
    unknowns = mode_coupling.shape[0]
    estimate = pl.CostEstimate(flops=1 << 30, bytes_accessed=1 << 21, transcendentals=1 << 18)
    invs, diags, ends, mode, waves, still, hat, along = pl.pallas_call(
        functools.partial(table_kernel, width=width, modes=modes),
        out_shape=[
            jax.ShapeDtypeStruct((4, width, width), BF16),
            jax.ShapeDtypeStruct((8, width), F32),
            jax.ShapeDtypeStruct((16, 4 * modes), F32),
            jax.ShapeDtypeStruct((2, unknowns, unknowns), BF16),
            jax.ShapeDtypeStruct((2, width, 4 * modes), F32),
            jax.ShapeDtypeStruct((2, width, width), F32),
            jax.ShapeDtypeStruct((2, 8 * modes, width), BF16),
            jax.ShapeDtypeStruct((2, 4 * modes, width), BF16),
        ],
        in_specs=[VMEM] * 8,
        out_specs=[VMEM] * 8,
        compiler_params=params(16),
        cost_estimate=estimate,
        name="tables",
    )(wave, mode_coupling, rows, lam_col, dirs, forcing, qh, ql)
    mine, invs, diags, ends, mode, waves, still, coupling, picks, hat, along = lax.optimization_barrier(
        (mine, invs, diags, ends, mode, waves, still, coupling, picks, hat, along)
    )
    other = lax.ppermute(mine, "row", [(a, a ^ 1) for a in range(na)])
    jumps, green, turned = pl.pallas_call(
        functools.partial(side_kernel, width=width, modes=modes),
        out_shape=[
            jax.ShapeDtypeStruct((2, 4 * width, 8 * modes), BF16),
            jax.ShapeDtypeStruct((4, width, width), F32),
            jax.ShapeDtypeStruct((2, width, 8 * modes), BF16),
        ],
        in_specs=[VMEM] * 7,
        out_specs=[VMEM] * 3,
        compiler_params=params(16),
        cost_estimate=estimate,
        name="sides",
    )(rows, col, hat, invs, diags, qh, ql)
    return pl.pallas_call(
        functools.partial(second_kernel, width=width, modes=modes, nb=nb),
        out_shape=jax.ShapeDtypeStruct((2, width, width), F32),
        in_specs=[VMEM, SMEM] + [VMEM] * 18,
        out_specs=VMEM,
        compiler_params=params(28),
        name="sweeps",
    )(wave, own, mine, other, coupling, picks, rows, hat, invs, diags, ends, mode, waves, still, jumps, green, turned, along, qh, ql)


def solution(mesh):
    return jax.shard_map(
        local,
        mesh=mesh,
        in_specs=(P(None, "row", "col"), P(), P(), P(), P(), P()),
        out_specs=P(None, "row", "col"),
        check_vma=False,
    )
```

```python
import functools
import math

import jax
import jax.numpy as jnp
import numpy as np
from jax import lax
from jax.experimental import pallas as pl
from jax.experimental.pallas import tpu as pltpu
from jax.sharding import PartitionSpec as P

ANGLES = 64
KAPPA_UNIT = 0.04
DAMPING = 0.5
F32 = jnp.float32
BF16 = jnp.bfloat16
NN = (((1,), (0,)), ((), ()))
NT = (((1,), (1,)), ((), ()))
TN = (((0,), (0,)), ((), ()))
VMEM = pl.BlockSpec(memory_space=pltpu.VMEM)
HBM = pl.BlockSpec(memory_space=pltpu.HBM)
SMEM = pl.BlockSpec(memory_space=pltpu.SMEM)


def split(a):
    if isinstance(a, tuple):
        return a
    high = a.astype(BF16)
    return high, (a - high.astype(F32)).astype(BF16)


def dot(a, b, dims=NN):
    ah, al = split(a)
    bh, bl = split(b)
    mul = functools.partial(lax.dot_general, dimension_numbers=dims, preferred_element_type=F32)
    (da,), (db,) = dims[0]
    size = ah.shape[1 - da]
    if size <= 224 and da == 1 and size % 8 == 0:
        both = mul(jnp.concatenate([ah.astype(F32), al.astype(F32)], 0).astype(BF16), bh)
        return both[:size] + (both[size:] + mul(ah, bl))
    if ah.shape[da] % 128 == 0:
        return mul(jnp.concatenate([ah, al, ah], da), jnp.concatenate([bh, bh, bl], db))
    return mul(ah, bh) + (mul(ah, bl) + mul(al, bh))


def cmul(a, b):
    return a[0] * b[0] - a[1] * b[1], a[0] * b[1] + a[1] * b[0]


def add(*terms):
    return sum(t[0] for t in terms[1:]) + terms[0][0], sum(t[1] for t in terms[1:]) + terms[0][1]


def sub(a, b):
    return a[0] - b[0], a[1] - b[1]


def sine_table(width):
    index = np.arange(1, width + 1)
    basis = np.sqrt(2.0 / (width + 1)) * np.sin(np.pi / (width + 1) * (np.outer(index, index) % (2 * width + 2)))
    values = 2.0 - 2.0 * np.cos(np.pi / (width + 1) * index)
    return basis.astype(np.float32), values.astype(np.float32)


def lanes(shape):
    return lax.broadcasted_iota(jnp.int32, shape, len(shape) - 1)


def parity(width):
    return (1 - 2 * (lanes((1, width)) & 1)).astype(F32)


def inverse_symbol(col_values, row_values, kappa):
    shift = kappa * kappa
    real = col_values + row_values - shift
    imag = DAMPING * shift
    norm = 1.0 / (real * real + imag * imag)
    return real * norm, imag * norm


def turn(z, half):
    sign = jnp.where(lanes((1, 2 * half)) < half, -1.0, 1.0)
    return sign * pltpu.roll(z, half, 1)


def contract(rows, table, dims=NT):
    count, half = rows[0].shape[0], table[0].shape[1 - dims[0][1][0]] // 2
    out = dot(jnp.concatenate(rows, 0), table, dims)
    return out[:count] + turn(out[count:], half)


def turn_column(dirs, modes):
    shape = (modes, modes)
    spot = lax.broadcasted_iota(jnp.int32, shape, 0) == lanes(shape)
    column = jnp.sum(jnp.where(spot, jnp.broadcast_to(dirs[...].astype(F32), shape), 0.0), 1, keepdims=True)
    return 2.0 * math.pi / ANGLES * column


def turn_row(dirs, modes):
    shape = (modes, 4 * modes)
    spot = (lax.broadcasted_iota(jnp.int32, shape, 0) == lanes(shape) % modes).astype(F32)
    row = lax.dot_general(
        jnp.broadcast_to(dirs[...].astype(F32), (8, modes)).astype(BF16), spot.astype(BF16), NN, preferred_element_type=F32
    )
    return 2.0 * math.pi / ANGLES * row[0:1]


def wave_table(kappa, theta, width):
    line = lanes((1, width)).astype(F32)
    ramp = (line + 0.5) / width
    windows = (1.0 - ramp, ramp)
    tables = []
    for speed in (jnp.cos(theta), jnp.sin(theta)):
        phase = kappa * speed * line
        cosine, sine = jnp.cos(phase), jnp.sin(phase)
        tables += [w * cosine for w in windows] + [-w * sine for w in windows]
    return jnp.concatenate(tables, 0)


def first_kernel(
    wave_in, dirs_in, forcing_in, qh_in, ql_in, rows_in, lam_in, payload,
    wave, dirs, forcing, qh, ql, rows, lam_col, arrived, *, width, modes
):
    sources = wave_in, dirs_in, qh_in, ql_in, forcing_in, rows_in, lam_in
    targets = wave, dirs, qh, ql, forcing, rows, lam_col
    copies = [pltpu.make_async_copy(a, b, arrived.at[k]) for k, (a, b) in enumerate(zip(sources, targets))]
    for copy in copies:
        copy.start()
    for copy in copies[:2]:
        copy.wait()
    kappa = KAPPA_UNIT * wave[...].astype(F32)
    table = wave_table(kappa, turn_column(dirs, modes), width)
    for copy in copies[2:]:
        copy.wait()
    basis = (qh[...], ql[...])
    hats = split(dot(table, basis))
    across_hat = hats[0][: 4 * modes], hats[1][: 4 * modes]
    along_hat = hats[0][4 * modes :], hats[1][4 * modes :]

    half_way = dot(forcing[...].reshape(2 * width, width), basis)
    coeff = [dot(basis, half_way[:width]), dot(basis, half_way[width:])]
    inv = inverse_symbol(lam_col[...], rows[4:5], kappa)
    coeff = [split(c) for c in cmul(coeff, inv)]
    weights = split(rows[...])
    out = []
    vectors = []
    for dims, table_hat in ((NN, along_hat), (NT, across_hat)):
        real, imag = dot(weights, coeff[0], dims), dot(weights, coeff[1], dims)
        edges = []
        for near, inner in ((0, 1), (2, 3)):
            e = real[near : near + 1], imag[near : near + 1]
            d = sub(e, (real[inner : inner + 1], imag[inner : inner + 1]))
            edges.append(e)
            vectors += [e[0] - kappa * d[1], e[1] + kappa * d[0]]
        rows_r = jnp.concatenate([edges[0][0], edges[1][0]] + [edges[0][0]] * 6, 0)
        rows_i = jnp.concatenate([edges[0][1], edges[1][1]] + [edges[0][1]] * 6, 0)
        proj = contract((rows_r, rows_i), table_hat)
        out += [proj[0:1], proj[1:2]]
    flat = jnp.concatenate(out + vectors, 1)
    payload[...] = jnp.broadcast_to(flat[None], payload.shape)


def spread(proj, side, ends, modes):
    half, lane = 2 * modes, lanes((1, 4 * modes))
    low = lane < half
    if side in "tb":
        real = jnp.where(low, proj, pltpu.roll(proj, half, 1))
        imag = jnp.where(low, pltpu.roll(proj, half, 1), proj)
    else:
        by1, by2, by3 = (pltpu.roll(proj, k * modes, 1) for k in (1, 2, 3))
        block = lane // modes
        real = jnp.where(block == 0, proj, jnp.where(block == 3, by2, by1))
        imag = jnp.where(block == 0, by2, jnp.where(block == 3, proj, by3))
    parts = cmul((real, imag), ends[side])
    return jnp.concatenate(parts, 1)


def table_kernel(
    wave, mode, rows, lam_col, dirs, forcing, qh, ql,
    inv_out, diag_out, ends_out, mode_out, wave_out, still, hat_out, along_out, *, width, modes
):
    kappa = KAPPA_UNIT * wave[...].astype(F32)
    half = 2 * modes
    inv = inverse_symbol(lam_col[...], rows[4:5], kappa)
    inv_split = split(inv[0]), split(inv[1])
    for part in range(2):
        for k in range(2):
            inv_out[2 * part + k] = inv_split[part][k]
    sign = parity(width)
    q0, q1 = rows[0:1], rows[1:2]
    diag_rows = split(jnp.concatenate([q0 * q0, sign * q0 * q0, q0 * (q0 - q1), sign * q0 * (q0 - q1)] * 2, 0))
    real, imag = dot(diag_rows, inv_split[0]), dot(diag_rows, inv_split[1])
    diag_out[...] = jnp.concatenate(
        [
            real[0:1], imag[0:1], real[1:2], imag[1:2],
            real[0:1] - kappa * imag[2:3], imag[0:1] + kappa * real[2:3],
            real[1:2] - kappa * imag[3:4], imag[1:2] + kappa * real[3:4],
        ],
        0,
    )

    basis = (qh[...], ql[...])
    half_way = dot(forcing[...].reshape(2 * width, width), basis)
    coeff = cmul((dot(basis, half_way[:width]), dot(basis, half_way[width:])), inv)
    for part in range(2):
        still[part] = dot(dot(basis, coeff[part]), basis)
    table = wave_table(kappa, turn_column(dirs, modes), width)
    along_out[0], along_out[1] = split(table[4 * modes :])
    hat_out[0], hat_out[1] = split(dot(table, basis))

    lane = lanes((1, 4 * modes))
    theta = turn_row(dirs, modes)
    speeds = jnp.cos(theta), jnp.sin(theta)
    pick = lane // half, (lane // modes) % 2

    def wave_at(axis, x):
        ramp = (x + 0.5) / width
        window = jnp.where(pick[axis] == 0, 1.0 - ramp, ramp)
        phase = kappa * speeds[axis] * float(x)
        return window * jnp.cos(phase), -window * jnp.sin(phase)

    ends = []
    for axis, near, inner in ((0, 0, 1), (0, width - 1, width - 2), (1, 0, 1), (1, width - 1, width - 2)):
        e, n = wave_at(axis, near), wave_at(axis, inner)
        er, ei, nr, ni = e[0], -e[1], n[0], -n[1]
        ends += [e[0], e[1], er - kappa * (ei - ni), ei + kappa * (er - nr)]
    ends_out[...] = jnp.concatenate(ends, 0)
    met = {side: (ends[4 * k], ends[4 * k + 1]) for k, side in enumerate("btrl")}
    shape = (4 * modes, 4 * modes)
    eye = (lax.broadcasted_iota(jnp.int32, shape, 0) == lanes(shape)).astype(F32)
    shares = jnp.concatenate([spread(eye, side, met, modes) for side in "tblr"], 0)
    mode_out[0], mode_out[1] = split(dot(shares, mode[...], NT))
    line = lax.broadcasted_iota(jnp.int32, (width, 1), 0).astype(F32)
    phase = kappa * speeds[0] * line
    wave_out[0], wave_out[1] = jnp.cos(phase), jnp.sin(phase)


def side_kernel(rows, cols, hats, invs, diag_rows, qh, ql, jump_out, green_out, turned_out, *, width, modes):
    half = 2 * modes
    inv_split = (invs[0], invs[1]), (invs[2], invs[3])
    sign = parity(width)
    q0 = rows[0:1]
    basis = (qh[...].astype(F32) + ql[...].astype(F32)) * q0
    pair = split(jnp.concatenate([basis, basis * sign], 0))
    for part in range(2):
        made = dot(pair, inv_split[part])
        green_out[part], green_out[2 + part] = made[:width], made[width:]
    table = hats[0].astype(F32) + hats[1].astype(F32)
    turned = table.T
    turned_out[0], turned_out[1] = split(turned)
    weighted = table * q0
    stacked = split(jnp.concatenate([weighted, weighted * sign], 0))
    real, imag = dot(inv_split[0], stacked, NT), dot(inv_split[1], stacked, NT)
    diag = diag_rows[...].T
    size = 2 * half
    for part, sources in enumerate(("tblr", "lrtb")):
        at = slice(size * part, size * part + size)
        blocks = {}
        for k, src in enumerate(sources[:2]):
            off = slice(at.start + 2 * size * k, at.stop + 2 * size * k)
            blocks[src] = (real[:, off] + turn(imag[:, off], half)) * cols[...]
        for k, src in enumerate(sources[2:]):
            blocks[src] = turned[:, at] * diag[:, 2 * k : 2 * k + 1] + turn(turned[:, at], half) * diag[:, 2 * k + 1 : 2 * k + 2]
        for k, src in enumerate("tblr"):
            high, low = split(blocks[src])
            jump_out[0, k * width : (k + 1) * width, at] = high
            jump_out[1, k * width : (k + 1) * width, at] = low


def second_kernel(
    wave, own, mine_in, other_in, coupling, picks, rows, hats, invs, diags, end_rows, mode, waves, still,
    jump_table, green, turned, along, qh, ql, field, *, width, modes, nb
):
    count = 2 * mine_in.shape[0]
    kappa = KAPPA_UNIT * wave[...].astype(F32)
    unknowns = 8 * modes
    half = 2 * modes
    lane = lanes((1, 4 * modes))
    inv_split = (invs[0], invs[1]), (invs[2], invs[3])
    sign = parity(width)
    q0, q1 = rows[0:1], rows[1:2]
    robin_weight = q0, kappa * (q0 - q1)
    same, opposite, same_robin, opposite_robin = ((diags[2 * k : 2 * k + 1], diags[2 * k + 1 : 2 * k + 2]) for k in range(4))
    across_hat = hats[0, : 2 * half], hats[1, : 2 * half]
    along_hat = hats[0, 2 * half :], hats[1, 2 * half :]
    across_turned = turned[0, :, : 2 * half], turned[1, :, : 2 * half]
    along_turned = turned[0, :, 2 * half :], turned[1, :, 2 * half :]
    tables = {"t": along_turned, "l": across_turned}
    mode_split = mode[0], mode[1]
    ends = {}
    for k, side in enumerate("tblr"):
        e = [end_rows[4 * k + j : 4 * k + j + 1] for j in range(4)]
        ends[side] = (e[0], e[1]), (e[2], e[3])
    facing = {"t": "b", "b": "t", "l": "r", "r": "l"}

    def outgoing(c, side):
        z = cmul((c[:, : unknowns // 2], c[:, unknowns // 2 :]), ends[side][1])
        low = lane < half
        if side in "tb":
            z = [a + pltpu.roll(a, half, 1) for a in z]
            z = jnp.where(low, z[0], z[1])
        else:
            z = [a + pltpu.roll(a, 3 * modes, 1) for a in z]
            block = lane // modes
            back = pltpu.roll(z[0], 3 * modes, 1)
            ahead = pltpu.roll(z[1], modes, 1)
            z = jnp.where(
                block == 0, z[0], jnp.where(block == 1, back, jnp.where(block == 2, pltpu.roll(z[1], 2 * modes, 1), ahead))
            )
        return z

    def synth(zs, table):
        size = zs[0].shape[0]
        stacked = jnp.concatenate([a for z in zs for a in (z, -turn(z, half))], 0)
        out = dot(stacked, table)
        return [(out[2 * k * size : (2 * k + 1) * size], out[(2 * k + 1) * size : (2 * k + 2) * size]) for k in range(len(zs))]

    def coarse_of(weights, projs):
        mixed = jnp.concatenate([dot(weights[k], projs[side]) for k, side in enumerate("tblr")], 1)
        return dot(mixed, mode_split)

    def robin_of(c, base):
        tb = synth([outgoing(c, "t"), outgoing(c, "b")], along_hat)
        lr = synth([outgoing(c, "l"), outgoing(c, "r")], across_hat)
        return {side: add(base[side], s) for side, s in zip("tblr", tb + lr)}

    row = lax.broadcasted_iota(jnp.int32, (count, 1), 0)
    first, last = row % nb == 0, row % nb == nb - 1

    def incoming(out):
        zero = jnp.zeros((nb, width), F32)
        down = lambda a: jnp.concatenate([zero, a[:-nb]], 0)
        up = lambda a: jnp.concatenate([a[nb:], zero], 0)
        right = lambda a: jnp.where(first, 0.0, pltpu.roll(a, 1, 0))
        left = lambda a: jnp.where(last, 0.0, pltpu.roll(a, count - 1, 0))
        move = lambda f, z: (f(z[0]), f(z[1]))
        return {"t": move(down, out["b"]), "b": move(up, out["t"]), "l": move(right, out["r"]), "r": move(left, out["l"])}

    def apply_inverse(vectors):
        size = vectors[0][0].shape[0]
        k = len(vectors)
        stacked = split(jnp.concatenate([v[0] for v in vectors] + [v[1] for v in vectors], 0))
        a, b = dot(stacked, inv_split[0]), dot(stacked, inv_split[1])
        real, imag = a[: k * size] - b[k * size :], a[k * size :] + b[: k * size]
        return [(real[j * size : (j + 1) * size], imag[j * size : (j + 1) * size]) for j in range(k)]

    def scale(r, z):
        return r * z[0], r * z[1]

    jump_split = jump_table[0], jump_table[1]

    def project_sources(rows_of):
        flip = lambda z: scale(sign, z)
        kinds = [
            [rows_of("lt", src) for src in "tblr"],
            [flip(rows_of("r", "t")), flip(rows_of("r", "b")), rows_of("r", "r"), rows_of("r", "l")],
            [rows_of("b", "b"), rows_of("b", "t"), flip(rows_of("b", "l")), flip(rows_of("b", "r"))],
        ]
        size = kinds[0][0][0].shape[0]
        stacked = jnp.concatenate([jnp.concatenate([z[part] for z in kind], 1) for part in range(2) for kind in kinds], 0)
        x = dot(stacked, jump_split)
        block = lambda k, at: (
            x[k * size : (k + 1) * size, at : at + 2 * half] + turn(x[(k + 3) * size : (k + 4) * size, at : at + 2 * half], half)
        )
        return {"l": block(0, 0), "t": block(0, 2 * half), "r": block(1, 0), "b": block(2, 2 * half)}

    def project_sent(sent):
        out = {}
        for a, b in (("t", "b"), ("l", "r")):
            size = sent[a][0].shape[0]
            both = contract([jnp.concatenate([sent[a][k], sent[b][k]], 0) for k in range(2)], tables[a], NN)
            out[a], out[b] = both[:size], both[size:]
        return out

    mine_rows, other_rows = (r[...].reshape(count // 2, r.shape[2]) for r in (mine_in, other_in))
    odd = own[0] // nb % 2 == 1
    low_rows, high_rows = jnp.where(odd, other_rows, mine_rows), jnp.where(odd, mine_rows, other_rows)
    values = jnp.concatenate([r[k : k + nb] for k in range(0, count // 2, nb) for r in (low_rows, high_rows)], 0)
    lanes_of = 4 * modes
    proj0 = {s: values[:, k * lanes_of : (k + 1) * lanes_of] for k, s in enumerate("tblr")}
    at = 4 * lanes_of
    robin0 = {}
    for s in "tblr":
        robin0[s] = values[:, at : at + width], values[:, at + width : at + 2 * width]
        at += 2 * width

    couplings = [split(coupling[k]) for k in range(4)]
    out1 = robin_of(coarse_of(couplings, proj0), robin0)
    g1 = incoming(out1)
    share, sent = project_sources(lambda o, src: g1[src]), project_sent(out1)
    proj1 = {s: proj0[s] + share[s] - sent[s] for s in "tblr"}
    pick = [split(picks[k]) for k in range(4)]
    base = {s: (dot(pick[k], robin0[s][0]), dot(pick[k], robin0[s][1])) for k, s in enumerate("tblr")}
    base_proj = {s: dot(pick[k], proj0[s]) for k, s in enumerate("tblr")}
    every = jnp.concatenate([picks[k] for k in range(4)], 0)
    every_split = split(every)
    mixed1 = {s: (dot(every_split, g1[s][0]), dot(every_split, g1[s][1])) for s in "tblr"}
    group = lambda z, k: (z[0][8 * k : 8 * k + 8], z[1][8 * k : 8 * k + 8])
    vectors = []
    for k, s in enumerate("tblr"):
        for src in "lr" if s in "tb" else "tb":
            z = cmul(group(mixed1[src], k), robin_weight)
            vectors.append(scale(sign, z) if s in "br" else z)
    x = apply_inverse(vectors)
    for k, s in enumerate("tblr"):
        cross = scale(q0, add(x[2 * k], scale(sign, x[2 * k + 1])))
        near, far = group(mixed1[s], k), group(mixed1[facing[s]], k)
        base[s] = add(base[s], cross, cmul(near, same_robin), cmul(far, opposite_robin))
    c1 = coarse_of([split(dot(every_split, couplings[k])) for k in range(4)], proj1)
    tb = synth([outgoing(c1[8 * k : 8 * k + 8], s) for k, s in ((0, "t"), (1, "b"))], along_hat)
    lr = synth([outgoing(c1[8 * k : 8 * k + 8], s) for k, s in ((2, "l"), (3, "r"))], across_hat)
    out2 = {s: add(base[s], z) for s, z in zip("tblr", tb + lr)}

    index = {"t": 0, "b": 1, "l": 2, "r": 3}
    rowof = lambda z, k: (z[0][k : k + 1], z[1][k : k + 1])

    share, sent = project_sources(lambda o, src: out2[facing[src]]), project_sent(out2)
    total = jnp.concatenate(
        [base_proj[o][5:6] + share[o][index[o] : index[o] + 1] - sent[o][5:6] for o in "tblr"], 1
    )
    c2 = dot(jnp.broadcast_to(total, (8, 16 * modes)), mode_split)[0:1]

    mine_g = {s: rowof(out2[facing[s]], 4) for s in "tblr"}
    basis = (qh[...], ql[...])
    near, far = (green[0], green[1]), (green[2], green[3])
    across_rows = add(cmul(near, mine_g["t"]), cmul(far, mine_g["b"]))
    across_cols = add(cmul(near, mine_g["l"]), cmul(far, mine_g["r"]))
    solved = [still[k] + dot(across_rows[k], basis) + dot(basis, across_cols[k], NT) for k in range(2)]

    cr, ci = c2[:, : 4 * modes], c2[:, 4 * modes :]
    low = lane < half
    flip = lambda a: pltpu.roll(a, half, 1)
    a0, a1 = jnp.where(low, cr, flip(ci)), jnp.where(low, flip(cr), ci)
    ramp = (lax.broadcasted_iota(jnp.int32, (width, 1), 0).astype(F32) + 0.5) / width
    blend = lambda lo, hi: lo + ramp * (hi - lo)
    v = waves[0] * blend(a0, a1) + waves[1] * blend(turn(a0, half), turn(a1, half))
    along_split = along[0], along[1]
    field[0] = solved[0] + dot(v, along_split)
    field[1] = solved[1] + dot(-turn(v, half), along_split)


def local(forcing, wave_index, directions, row_coupling, col_coupling, mode_coupling):
    width = forcing.shape[1]
    modes = directions.shape[0]
    na, nb = row_coupling.shape[0], col_coupling.shape[0]
    count = na * nb
    size = 4 * 4 * modes + 4 * 2 * width
    basis, values = sine_table(width)
    qh = basis.astype(jnp.bfloat16)
    ql = (basis - qh.astype(np.float32)).astype(jnp.bfloat16)
    sign = 1.0 - 2.0 * (np.arange(width) % 2)
    rows = np.zeros((8, width), np.float32)
    rows[0], rows[1], rows[2], rows[3], rows[4] = basis[0], basis[1], sign * basis[0], sign * basis[1], values
    lam_col, col = values[:, None], basis[0][:, None]
    wave, dirs = wave_index.reshape(1, 1), directions.reshape(1, modes)

    scale = 1.0 / math.sqrt(width) / math.sqrt(modes)
    rc, cc = row_coupling * scale, col_coupling
    pad = lambda m, lo: jnp.pad(m[:, :-1] if lo else m[:, 1:], ((0, 0), (1, 0) if lo else (0, 1)))
    kron = lambda a, b: (a[:, None, :, None] * b[None, :, None, :]).reshape(count, count)
    coupling = jnp.stack([kron(pad(rc, True), cc), kron(pad(rc, False), cc), kron(rc, pad(cc, True)), kron(rc, pad(cc, False))])
    own = (lax.axis_index("row") * nb + lax.axis_index("col")).reshape(1)
    tile = jnp.arange(count)
    taken = lax.dynamic_slice_in_dim(coupling, own[0], 1, 1)[:, 0]
    sums = jnp.concatenate([taken, (tile == own[0]).astype(F32)[None]])
    ahead = lambda m, by: jnp.pad(m[:, by:], ((0, 0), (0, by)))
    behind = lambda m, by: jnp.pad(m[:, :-by], ((0, 0), (by, 0)))
    moved = jnp.stack(
        [
            behind(sums, nb),
            ahead(sums, nb),
            jnp.where(tile % nb == 0, 0.0, behind(sums, 1)),
            jnp.where(tile % nb == nb - 1, 0.0, ahead(sums, 1)),
        ]
    )
    picks = jnp.concatenate([moved, taken[:, None], jnp.zeros((4, 2, count), F32)], 1)

    fits = count <= 64
    params = lambda mib: pltpu.CompilerParams(vmem_limit_bytes=mib << 20) if fits else None
    payload = pl.pallas_call(
        functools.partial(first_kernel, width=width, modes=modes),
        out_shape=jax.ShapeDtypeStruct((count // 2, 1, size), F32),
        in_specs=[HBM] * 7,
        out_specs=VMEM,
        scratch_shapes=[
            pltpu.VMEM((1, 1), jnp.int32),
            pltpu.VMEM((1, modes), jnp.int32),
            pltpu.VMEM((2, width, width), F32),
            pltpu.VMEM((width, width), BF16),
            pltpu.VMEM((width, width), BF16),
            pltpu.VMEM((8, width), F32),
            pltpu.VMEM((width, 1), F32),
            pltpu.SemaphoreType.DMA((7,)),
        ],
        name="spectrum",
    )(wave, dirs, forcing, qh, ql, rows, lam_col)
    groups = [[a * nb + b for a in range(k, na, 2) for b in range(nb)] for k in range(2)]
    mine = lax.all_to_all(payload, ("row", "col"), 0, 0, axis_index_groups=groups, tiled=True)
    unknowns = mode_coupling.shape[0]
    estimate = pl.CostEstimate(flops=1 << 30, bytes_accessed=1 << 21, transcendentals=1 << 18)
    invs, diags, ends, mode, waves, still, hat, along = pl.pallas_call(
        functools.partial(table_kernel, width=width, modes=modes),
        out_shape=[
            jax.ShapeDtypeStruct((4, width, width), BF16),
            jax.ShapeDtypeStruct((8, width), F32),
            jax.ShapeDtypeStruct((16, 4 * modes), F32),
            jax.ShapeDtypeStruct((2, 16 * modes, unknowns), BF16),
            jax.ShapeDtypeStruct((2, width, 4 * modes), F32),
            jax.ShapeDtypeStruct((2, width, width), F32),
            jax.ShapeDtypeStruct((2, 8 * modes, width), BF16),
            jax.ShapeDtypeStruct((2, 4 * modes, width), BF16),
        ],
        in_specs=[VMEM] * 8,
        out_specs=[VMEM] * 8,
        compiler_params=params(16),
        cost_estimate=estimate,
        name="tables",
    )(wave, mode_coupling, rows, lam_col, dirs, forcing, qh, ql)
    mine, invs, diags, ends, mode, waves, still, coupling, picks, hat, along = lax.optimization_barrier(
        (mine, invs, diags, ends, mode, waves, still, coupling, picks, hat, along)
    )
    other = lax.ppermute(mine, "row", [(a, a ^ 1) for a in range(na)])
    jumps, green, turned = pl.pallas_call(
        functools.partial(side_kernel, width=width, modes=modes),
        out_shape=[
            jax.ShapeDtypeStruct((2, 4 * width, 8 * modes), BF16),
            jax.ShapeDtypeStruct((4, width, width), F32),
            jax.ShapeDtypeStruct((2, width, 8 * modes), BF16),
        ],
        in_specs=[VMEM] * 7,
        out_specs=[VMEM] * 3,
        compiler_params=params(16),
        cost_estimate=estimate,
        name="sides",
    )(rows, col, hat, invs, diags, qh, ql)
    return pl.pallas_call(
        functools.partial(second_kernel, width=width, modes=modes, nb=nb),
        out_shape=jax.ShapeDtypeStruct((2, width, width), F32),
        in_specs=[VMEM, SMEM] + [VMEM] * 18,
        out_specs=VMEM,
        compiler_params=params(28),
        name="sweeps",
    )(wave, own, mine, other, coupling, picks, rows, hat, invs, diags, ends, mode, waves, still, jumps, green, turned, along, qh, ql)


def solution(mesh):
    return jax.shard_map(
        local,
        mesh=mesh,
        in_specs=(P(None, "row", "col"), P(), P(), P(), P(), P()),
        out_specs=P(None, "row", "col"),
        check_vma=False,
    )
```
